32 devices in a mesh: dp: 8 (over y, x, core), mp: 4 (over z).
Axes of the slice: x: 2, y: 2, z: 4, core: 2. Of those that a mesh axis runs over, the one named last changes fastest.
Arguments:
- states: bfloat16 [128, 80, 768], P('dp'), may hold values from -6 to 6
- hist_len: int32 [128], P('dp'), may hold values from 1 to 20
- norm_gain: float32 [768], replicated, may hold values from 0.5 to 1.5
- qkv_weight: bfloat16 [768, 3, 12, 64], P(None, None, 'mp'), may hold values from -1 to 1
- output_weight: bfloat16 [12, 64, 768], P('mp'), may hold values from -0.21875 to 0.21875
- cotangent: bfloat16 [128, 80, 768], P('dp'), may hold values from -6 to 6
Outputs:
- attended: bfloat16 [128, 80, 768], P('dp')
- grad_states: bfloat16 [128, 80, 768], P('dp')
- grad_qkv: float32 [768, 3, 12, 64], P('dp', None, 'mp')
- output_weight_gradient: float32 [12, 64, 768], P('mp', None, 'dp')
- grad_gain: float32 [768], P('dp')
The draws below stay inside these ranges and needn't reach their ends.
All inputs are finite; a program needn't handle non-finite values.
Results may differ from the reference program's by a relative error of at most 0.012.
Values may be sent and summed in bfloat16 or wider, within the bound.
A program may use at most 128 MiB of HBM per device.

```python
import jax
import jax.numpy as jnp
from jax import lax

D = 768
H = 12
DH = 64
ITEMS = 20
LEVELS = 4
S = 80
B = 128


def draw_qkv_weight(key, part):
    k_base, k_noise, k_value = jax.random.split(key, 3)
    inverse = D ** (-0.5)
    query_part = 0.5 * inverse * jax.random.normal(k_base, (D, H, DH), jnp.float32)
    key_part = 0.5 * inverse * jax.random.normal(k_noise, (D, H, DH), jnp.float32)
    value_part = inverse * jax.random.normal(k_value, (D, H, DH), jnp.float32)
    stacked = jnp.stack([query_part, key_part, value_part], axis=1)
    return jnp.clip(stacked, -1.0, 1.0).astype(jnp.bfloat16)


def set_ends(drawn, own_key, least, high):
    longest = drawn.shape.index(max(drawn.shape))
    spots = []
    for shift in (0, 1):
        where = [jax.random.randint(jax.random.fold_in(own_key, axis), (), 0, length) for axis, length in enumerate(drawn.shape)]
        where[longest] = (where[longest] + shift) % drawn.shape[longest]
        spots.append(tuple(where))
    return drawn.at[spots[0]].set(least).at[spots[1]].set(high)


def with_spikes(drawn, key, source, target, blocks, factor):
    def block_of(dim):
        return (jnp.arange(drawn.shape[dim]) // (drawn.shape[dim] // blocks)).reshape((-1,) + (1,) * (drawn.ndim - 1 - dim))

    first = jax.random.permutation(key, blocks)[block_of(target)]
    far = (block_of(target) + blocks // 2) % blocks
    return jnp.where((block_of(source) == first) | (block_of(source) == far), factor * drawn, drawn)


def block_levels(stream_key, extent, cuts, smallest, high):
    level, own = 1.0, jax.random.fold_in(stream_key, 6)
    for dim, blocks in cuts:
        heights = jnp.exp(jax.random.uniform(jax.random.fold_in(own, dim), (blocks,), jnp.float32, smallest / len(cuts), high / len(cuts)))
        level = level * jnp.repeat(heights, extent[dim] // blocks).reshape([-1 if axis == dim else 1 for axis in range(len(extent))])
    return level


def gaussian(own_key, shape, deviation, limit, pieces=(), kind=jnp.bfloat16):
    array = jax.random.normal(own_key, shape, jnp.float32) * deviation
    if len(pieces) > 0:
        array = block_levels(own_key, shape, pieces, -0.22, 0.18) * array
    return jnp.clip(array, min=-limit, max=limit).astype(kind)


def gaussian_with(rng, shape, deviation, reach, cuts, heavy, kind=jnp.bfloat16):
    result = deviation * jax.random.normal(rng, shape, jnp.float32)
    if cuts:
        result = result * block_levels(rng, shape, cuts, -0.22, 0.18)
    return jnp.clip(with_spikes(result, jax.random.fold_in(rng, 3), *heavy), -reach, reach).astype(kind)


def setup_inputs(seed: int = 0) -> dict:
    keys = jax.random.split(jax.random.key(seed), 7)
    states = gaussian_with(keys[0], (B, S, D), 1.0, 6.0, ((0, 8),), (0, 2, 8, 2.0))
    hist_len = set_ends(jax.random.randint(keys[1], (B,), 1, ITEMS + 1), jax.random.fold_in(keys[1], 1), 1, ITEMS).astype(jnp.int32)
    norm_gain = jnp.clip(1.0 + 0.1 * jax.random.normal(keys[2], (D,), jnp.float32), 0.5, 1.5)
    qkv_weight = draw_qkv_weight(jax.random.fold_in(keys[6], 71), 0)
    output_weight = gaussian(keys[4], (H, DH, D), (H * DH) ** -0.5, 0.21875, ((0, 4),))
    cotangent = gaussian_with(keys[5], (B, S, D), 1.0, 6.0, ((0, 8),), (0, 2, 8, 2.0))
    return {"states": states, "hist_len": hist_len, "norm_gain": norm_gain, "qkv_weight": qkv_weight, "output_weight": output_weight, "cotangent": cotangent}


def reference(states, hist_len, norm_gain, qkv_weight, output_weight, cotangent):
    wide_states = states.astype(jnp.float32)
    inv_rms = lax.rsqrt(lax.optimization_barrier(jnp.mean(wide_states * wide_states, axis=-1, keepdims=True)) + 1e-06)
    unit = wide_states * inv_rms
    normed = (unit * norm_gain).astype(jnp.bfloat16)
    proj = jnp.einsum('bsd,dchk->bschk', normed.astype(jnp.float32), qkv_weight.astype(jnp.float32)).astype(jnp.bfloat16)
    queries = proj[:, :, 0].astype(jnp.float32)
    key_rows = proj[:, :, 1].astype(jnp.float32)
    value_rows = proj[:, :, 2].astype(jnp.float32)
    positions = jnp.arange(states.shape[1], dtype=jnp.int32)
    keep_mask = positions[None, :] < LEVELS * hist_len[:, None]
    scores = jnp.einsum('bqhk,bphk->bhqp', queries, key_rows)
    masked = jnp.where(keep_mask[:, None, None, :], scores, -1e+30)
    row_top = lax.optimization_barrier(jnp.max(masked, axis=-1, keepdims=True))
    exp_scores = jnp.exp(masked - row_top)
    attn_prob = exp_scores / lax.optimization_barrier(jnp.sum(exp_scores, axis=-1, keepdims=True))
    prob_bf = attn_prob.astype(jnp.bfloat16).astype(jnp.float32)
    attended_context = jnp.einsum('bhqp,bphk->bqhk', prob_bf, value_rows).astype(jnp.bfloat16)
    mixed_total_sum = jnp.einsum('zagm,gms->zas', attended_context.astype(jnp.float32), output_weight.astype(jnp.float32))
    attended = (wide_states + mixed_total_sum).astype(jnp.bfloat16)
    masked_cotangent = jnp.where(keep_mask[:, :, None], cotangent, jnp.zeros_like(cotangent)).astype(jnp.float32)
    output_weight_gradient = jnp.einsum('wmep,wmx->epx', attended_context.astype(jnp.float32), masked_cotangent)
    context_gradient = jnp.einsum('uxy,wgy->uxwg', masked_cotangent, output_weight.astype(jnp.float32)).astype(jnp.bfloat16).astype(jnp.float32)
    grad_prob = jnp.einsum('bqhk,bphk->bhqp', context_gradient, value_rows)
    row_delta = lax.optimization_barrier(jnp.sum(attn_prob * grad_prob, axis=-1, keepdims=True))
    grad_score = (attn_prob * (grad_prob - row_delta)).astype(jnp.bfloat16).astype(jnp.float32)
    grad_query = jnp.einsum('bhqp,bphk->bqhk', grad_score, key_rows)
    grad_key = jnp.einsum('bhqp,bqhk->bphk', grad_score, queries)
    grad_value = jnp.einsum('bhqp,bqhk->bphk', prob_bf, context_gradient)
    grad_proj = jnp.stack([grad_query, grad_key, grad_value], axis=2).astype(jnp.bfloat16).astype(jnp.float32)
    grad_qkv = jnp.einsum('bsd,bschk->dchk', normed.astype(jnp.float32), grad_proj)
    grad_normed = jnp.einsum('bschk,dchk->bsd', grad_proj, qkv_weight.astype(jnp.float32))
    grad_gain = lax.optimization_barrier(jnp.sum(grad_normed * unit, axis=(0, 1)))
    grad_unit = grad_normed * norm_gain
    row_corr = lax.optimization_barrier(jnp.mean(grad_unit * unit, axis=-1, keepdims=True))
    grad_states = (masked_cotangent + inv_rms * (grad_unit - unit * row_corr)).astype(jnp.bfloat16)
    return (attended, grad_states, grad_qkv, output_weight_gradient, grad_gain)
```

```python
import functools

import jax
import jax.numpy as jnp
from jax import lax
from jax.experimental import pallas as pl
from jax.experimental.pallas import tpu as pltpu
from jax.sharding import PartitionSpec as P

LEVELS = 4
NB = 4
WIN = 256
BF = jnp.bfloat16
F32 = jnp.float32
MESH = pl.DeviceIdType.MESH


def dot(a, b, ca, cb):
    return lax.dot_general(a, b, (((ca,), (cb,)), ((), ())), preferred_element_type=F32)


def kernel(n, nd, s, hist, states, cot, gain, wqkv, wout, att, gst, gq, go, gg,
           wall, st, mc, normed, inv, pj, sq, sg, scb, gpb, pbb, dsb, ctx, gproj,
           part, got, total, held, tot, zz, res, gqv, gov, ggv,
           s_w, s_in, s_out, s_res, s_z, r_z, s_x, r_x, s_d, r_d, s_c, r_c, s_p, r_p, s_o, r_o, s_g, r_g):
    rows_all, dim = st.shape
    width = wout.shape[0]
    rows = NB * s
    nblk = rows_all // rows
    half = nd // 2
    piece = dim // nd
    d, z = lax.axis_index("dp"), lax.axis_index("mp")
    c, chip = d % 2, d // 2
    bx, by = chip % 2, (chip // 2) % 2
    partner = (d + 1 - 2 * c, z)
    across = ((d + 2 - 4 * bx, z), (d + 4 - 8 * by, z))
    others = [(((chip + o) % half) * 2 + c, z) for o in range(1, half)]
    zpeers = [(d, (z + n - j) % n) for j in range(1, n)]

    loads = []
    for k in range(3):
        loads.append(pltpu.make_async_copy(
            wqkv.at[pl.ds(k * width, width)], wall.at[pl.ds(k * dim, width)], s_w.at[k]))
    loads.append(pltpu.make_async_copy(wout, wall.at[pl.ds(3 * dim, width)], s_w.at[3]))
    for copy in loads:
        copy.start()
    for i in range(nblk):
        at = pl.ds(i * rows, rows)
        pltpu.make_async_copy(states.at[at], st.at[at], s_in.at[0, i]).start()
        pltpu.make_async_copy(cot.at[at], mc.at[at], s_in.at[1, i]).start()

    barrier = pltpu.get_barrier_semaphore()
    greet = zpeers + others + [partner]
    for device in greet:
        pl.semaphore_signal(barrier, inc=1, device_id=device, device_id_type=MESH)
    pj[...] = jnp.zeros_like(pj)
    sq[...] = jnp.zeros_like(sq)
    sg[...] = jnp.zeros_like(sg)
    for copy in loads:
        copy.wait()
    pl.semaphore_wait(barrier, len(greet))

    def remote(src, dst, ssem, rsem, device):
        return pltpu.make_async_remote_copy(
            src_ref=src, dst_ref=dst, send_sem=ssem, recv_sem=rsem, device_id=device, device_id_type=MESH
        )

    def arrived(spot, rsem):
        remote(spot, spot, rsem, rsem, partner).wait_recv()

    quarter = width // 4

    def spot(j, x, y, core, i=0, count=2):
        first = pl.multiple_of((x + 2 * y) * dim + place[j] * width + (2 * core + i) * quarter, 16)
        return wall.at[pl.ds(first, count * quarter)]

    order = [j for j in (1, n - 1) if j < n] + [j for j in range(2, n - 1)]
    place = {j: m for m, j in enumerate([0] + order)}

    def send_own():
        mine = spot(0, bx, by, c)
        for j in order:
            remote(mine, spot(j, bx, by, c), s_z.at[j - 1], r_z.at[j - 1], zpeers[j - 1]).start()

    def first_hop(j):
        here = spot(j, bx, by, c)
        arrived(here, r_z.at[j - 1])
        for i in range(2):
            remote(here, here, s_x.at[i, j - 1], r_x.at[i, j - 1], across[i]).start()
        remote(here, here, s_c.at[0, j - 1], r_c.at[0, j - 1], partner).start()

    sides = ((1 - bx, by), (bx, 1 - by))
    diag = (1 - bx, 1 - by)

    def second_hop(j):
        for i in range(2):
            here = spot(j, *sides[i], c)
            arrived(here, r_x.at[i, j - 1])
            one = spot(j, *sides[i], c, i, 1)
            remote(one, one, s_d.at[i, j - 1], r_d.at[i, j - 1], across[1 - i]).start()
            remote(here, here, s_c.at[1 + i, j - 1], r_c.at[1 + i, j - 1], partner).start()

    def third_hop(j):
        for i in range(2):
            one = spot(j, *diag, c, i, 1)
            arrived(one, r_d.at[i, j - 1])
            remote(one, one, s_c.at[3 + i, j - 1], r_c.at[3 + i, j - 1], partner).start()

    def landed(j):
        for k, (x, y) in enumerate(((bx, by),) + sides):
            arrived(spot(j, x, y, 1 - c), r_c.at[k, j - 1])
        for i in range(2):
            arrived(spot(j, *diag, 1 - c, i, 1), r_c.at[3 + i, j - 1])

    scatter_order = list(range(1, half)) + [0]

    def scatter_core():
        for o in scatter_order:
            t = (chip + o) % half
            remote(part.at[1 - c, t], got.at[o], s_p.at[o], r_p.at[o], partner).start()

    def scatter_chip():
        for o in scatter_order:
            t = (chip + o) % half
            arrived(got.at[o], r_p.at[o])
            both = part[c, t].astype(F32) + got[o].astype(F32)
            if o == 0:
                tot[:piece, :] = both
            else:
                total[o - 1] = both.astype(BF)
                remote(total.at[o - 1], held.at[o - 1], s_o.at[o - 1], r_o.at[o - 1], others[o - 1]).start()

    def scatter_sum():
        for o in range(1, half):
            arrived(held.at[o - 1], r_o.at[o - 1])
            tot[:piece, :] += held[o - 1].astype(F32)
        column = lax.broadcasted_iota(jnp.int32, (dim, 128), 1)
        row = lax.broadcasted_iota(jnp.int32, (dim, 128), 0)
        pick = (row - piece * d == column).astype(F32).astype(BF)
        gsum = jnp.zeros((1, 128), F32)
        for k in range(4):
            turned = tot[:, k * WIN : (k + 1) * WIN].T[:width]
            if k < 3:
                gqv[k * width : (k + 1) * width, :] = turned[:, :piece]
                mine = dot(wall[k * dim : k * dim + width, :], pick, 1, 0)
                gsum = gsum + jnp.sum(mine * turned, axis=0, keepdims=True)
            else:
                gov[...] = turned[:, :piece]
        scale = gain[...]
        own_gain = jnp.ones((1, piece), F32)
        for t in range(nd):
            own_gain = jnp.where(d == t, scale[:, t * piece : (t + 1) * piece], own_gain)
        zz[z, 0:1, :piece] = gsum[:, :piece] / own_gain
        for j in range(1, n):
            remote(zz.at[z], zz.at[z], s_g.at[j - 1], r_g.at[j - 1], zpeers[j - 1]).start()
        pltpu.make_async_copy(gqv, gq, s_res.at[0]).start()
        pltpu.make_async_copy(gov, go, s_res.at[1]).start()

    def gain_sum():
        for j in range(1, n):
            arrived(zz.at[(z + j) % n], r_g.at[j - 1])
        value = zz[0, 0:1, :piece]
        for k in range(1, n):
            value = value + zz[k, 0:1, :piece]
        ggv[...] = value
        pltpu.make_async_copy(ggv, gg, s_res.at[2]).start()

    lane = lax.broadcasted_iota(jnp.int32, (s, 128), 1)
    low = (lane < 64).astype(F32).astype(BF)
    high = (lane >= 64).astype(F32).astype(BF)
    key_pos = lax.broadcasted_iota(jnp.int32, (s, WIN), 0)

    def spread(x, out, odd):
        left, right = x[:, :128], x[:, 128:]
        if odd:
            out[0:s, :128] = left * high
            out[s : 2 * s, 128:] = right * low
            out[2 * s : 3 * s, 128:] = right * high
        else:
            out[0:s, :128] = left * low
            out[s : 2 * s, :128] = left * high
            out[2 * s : 3 * s, 128:] = right * low

    def fold(x, odd):
        a, b, e = x[:s], x[s : 2 * s], x[2 * s : 3 * s]
        if odd:
            left = jnp.where(lane < 64, 0.0, a[:, :128])
            right = jnp.where(lane < 64, b[:, 128:], e[:, 128:])
        else:
            left = jnp.where(lane < 64, a[:, :128], b[:, :128])
            right = jnp.where(lane < 64, e[:, 128:], 0.0)
        return jnp.concatenate([left, right], axis=1)

    def put(ref, at, base, x, odd):
        x = x.astype(BF)
        if odd:
            ref[at, base + 128 : base + 256] += x[:, :128]
            ref[at, base + 256 : base + 384] = x[:, 128:]
        else:
            ref[at, base : base + 256] = x

    def prepare(i):
        at = pl.ds(pl.multiple_of(i * rows, 16), rows)
        pltpu.make_async_copy(states.at[at], st.at[at], s_in.at[0, i]).wait()
        pltpu.make_async_copy(cot.at[at], mc.at[at], s_in.at[1, i]).wait()
        wide = st[at, :].astype(F32)
        scale = lax.rsqrt(jnp.mean(wide * wide, axis=-1, keepdims=True) + 1e-06)
        inv[at, :] = scale
        normed[at, :] = (wide * scale * gain[...]).astype(BF)
        pos = lax.broadcasted_iota(jnp.int32, (s, dim), 0)
        for b in range(NB):
            one = pl.ds(pl.multiple_of(i * rows + b * s, 16), s)
            keep = pos < LEVELS * hist[i * NB + b]
            mc[one, :] = jnp.where(keep, mc[one, :].astype(F32), 0.0).astype(BF)

    def attention(slot, i):
        odd = slot % 2
        base = 2 * width * (slot // 2)
        first = slot * width - 64 * odd
        cols = width + 64 * odd
        at = pl.ds(pl.multiple_of(i * rows, 16), rows)
        for k in range(4):
            lhs = normed[at, :] if k < 3 else mc[at, :]
            pj[k, :, :cols] = dot(lhs, wall[k * dim + first : k * dim + first + cols, :], 1, 1).astype(BF)

        def scores(b):
            mine = slice(b * s, (b + 1) * s)
            spread(pj[0, mine, :], sq.at[odd, b], odd)
            spread(pj[3, mine, :], sg.at[odd, b], odd)
            scb[b] = dot(pj[1, mine, :], sq[odd, b], 1, 1)
            gpb[b] = dot(pj[2, mine, :], sg[odd, b], 1, 1)

        def soft(b):
            keep = key_pos < LEVELS * hist[i * NB + b]
            sc = jnp.where(keep, scb[b], -1e30)
            ex = jnp.exp(sc - jnp.max(sc, axis=0, keepdims=True))
            prob = ex * (1.0 / jnp.sum(ex, axis=0, keepdims=True))
            pbb[b] = prob.astype(BF)
            gp = gpb[b]
            delta = jnp.sum(prob * gp, axis=0, keepdims=True)
            dsb[b] = (prob * (gp - delta)).astype(BF)

        def outs(b):
            mine = slice(b * s, (b + 1) * s)
            one = pl.ds(pl.multiple_of(i * rows + b * s, 16), s)
            pb, ds = pbb[b], dsb[b]
            put(gproj, one, dim + base, dot(ds, sq[odd, b], 1, 0), odd)
            put(gproj, one, 2 * dim + base, dot(pb, sg[odd, b], 1, 0), odd)
            put(ctx, one, base, fold(dot(pb, pj[2, mine, :], 0, 0), odd), odd)
            put(gproj, one, base, fold(dot(ds, pj[1, mine, :], 0, 0), odd), odd)

        scores(0)
        scores(1)
        for b in range(NB):
            soft(b)
            if b + 2 < NB:
                scores(b + 2)
            outs(b)

    def weight_grads():
        for k in range(4):
            lhs = normed[...] if k < 3 else mc[...]
            rhs = gproj[:, k * dim : k * dim + WIN] if k < 3 else ctx[:, :WIN]
            acc = dot(lhs, rhs, 0, 0)
            for t in range(nd):
                part[t % 2, t // 2, :, k * WIN : (k + 1) * WIN] = acc[t * piece : (t + 1) * piece].astype(BF)

    def results(i):
        at = pl.ds(pl.multiple_of(i * rows, 16), rows)
        wide = st[at, :].astype(F32)
        copies = [
            pltpu.make_async_copy(res.at[k, i % 2], (att, gst)[k].at[at], s_out.at[k, i % 2]) for k in range(2)
        ]

        @pl.when(i >= 2)
        def _():
            for copy in copies:
                copy.wait()

        res[0, i % 2] = (wide + dot(ctx[at, :], wall[3 * dim :, :], 1, 0)).astype(BF)
        gn = dot(gproj[at, :], wall[: 3 * dim, :], 1, 0)
        scale = inv[at, :]
        unit = wide * scale
        gu = gn * gain[...]
        corr = jnp.mean(gu * unit, axis=-1, keepdims=True)
        res[1, i % 2] = (mc[at, :].astype(F32) + scale * (gu - unit * corr)).astype(BF)
        for copy in copies:
            copy.start()

    def at_step(i, steps):
        for k, step in enumerate(steps):
            if step:
                @pl.when(i == k)
                def _():
                    for one in step:
                        one()

    plan = {stage: [[] for _ in range(nblk)] for stage in range(n)}

    def note(stage, i, step, *args):
        spots = [(a, b) for a in range(n) for b in range(nblk)]
        place = min(stage * nblk + i, len(spots) - 1)
        a, b = spots[place]
        plan[a][b].append(functools.partial(step, *args))

    tail = []
    for m, j in enumerate(order):
        begin = m * nblk
        note(0, begin + 1, first_hop, j)
        note(0, begin + 2, second_hop, j)
        note(0, begin + 3, third_hop, j)
        plan[m + 1][0].insert(0, functools.partial(landed, j))
    note(1, 1, scatter_chip)
    note(2, 1, scatter_sum)
    note(3, 1, gain_sum)

    send_own()
    for m in range(n):
        @pl.loop(0, nblk)
        def _(i):
            at_step(i, plan[m])
            if m == 0:
                prepare(i)
            attention(m, i)
        if m == 0:
            weight_grads()
            scatter_core()

    pl.loop(0, nblk)(results)

    for i in range(max(nblk - 2, 0), nblk):
        at = pl.ds(i * rows, rows)
        for k in range(2):
            pltpu.make_async_copy(res.at[k, i % 2], (att, gst)[k].at[at], s_out.at[k, i % 2]).wait()
    pltpu.make_async_copy(gqv, gq, s_res.at[0]).wait()
    pltpu.make_async_copy(gov, go, s_res.at[1]).wait()
    pltpu.make_async_copy(ggv, gg, s_res.at[2]).wait()

    def sent(src, ssem):
        remote(src, src, ssem, ssem, partner).wait_send()

    for j in order:
        here = spot(j, bx, by, c)
        sent(here, s_z.at[j - 1])
        sent(here, s_c.at[0, j - 1])
        for i in range(2):
            sent(here, s_x.at[i, j - 1])
            sent(here, s_c.at[1 + i, j - 1])
            sent(spot(j, bx, by, c, 0, 1), s_d.at[i, j - 1])
            sent(spot(j, bx, by, c, 0, 1), s_c.at[3 + i, j - 1])
        sent(zz.at[0], s_g.at[j - 1])
    for o in range(half):
        sent(got.at[o], s_p.at[o])
    for o in range(1, half):
        sent(held.at[o - 1], s_o.at[o - 1])


def body(nd, n, states, hist_len, norm_gain, qkv_weight, output_weight, cotangent):
    dim, _, heads, size = qkv_weight.shape
    count, s, _ = states.shape
    width = heads * size
    total = count * s
    rows = NB * s
    nblk = count // NB
    half = nd // 2
    piece = dim // nd
    wqkv = qkv_weight.transpose(1, 2, 3, 0).reshape(3 * width, dim)
    wout = output_weight.reshape(width, dim)
    anywhere = pl.BlockSpec(memory_space=pl.ANY)
    dma = pltpu.SemaphoreType.DMA
    att, gst, gq, go, gg = pl.pallas_call(
        functools.partial(kernel, n, nd, s),
        out_shape=(
            jax.ShapeDtypeStruct((total, dim), BF),
            jax.ShapeDtypeStruct((total, dim), BF),
            jax.ShapeDtypeStruct((3 * width, piece), F32),
            jax.ShapeDtypeStruct((width, piece), F32),
            jax.ShapeDtypeStruct((1, piece), F32),
        ),
        in_specs=[
            pl.BlockSpec(memory_space=pltpu.SMEM),
            anywhere,
            anywhere,
            pl.BlockSpec(memory_space=pltpu.VMEM),
            anywhere,
            anywhere,
        ],
        out_specs=(anywhere,) * 5,
        scratch_shapes=[
            pltpu.VMEM((4 * dim, dim), BF),
            pltpu.VMEM((total, dim), BF),
            pltpu.VMEM((total, dim), BF),
            pltpu.VMEM((total, dim), BF),
            pltpu.VMEM((total, 1), F32),
            pltpu.VMEM((4, rows, WIN), BF),
            pltpu.VMEM((2, NB, WIN, WIN), BF),
            pltpu.VMEM((2, NB, WIN, WIN), BF),
            pltpu.VMEM((NB, s, WIN), F32),
            pltpu.VMEM((NB, s, WIN), F32),
            pltpu.VMEM((NB, s, WIN), BF),
            pltpu.VMEM((NB, s, WIN), BF),
            pltpu.VMEM((total, dim), BF),
            pltpu.VMEM((total, 3 * dim), BF),
            pltpu.VMEM((2, half, piece, 4 * WIN), BF),
            pltpu.VMEM((half, piece, 4 * WIN), BF),
            pltpu.VMEM((half - 1, piece, 4 * WIN), BF),
            pltpu.VMEM((half - 1, piece, 4 * WIN), BF),
            pltpu.VMEM((128, 4 * WIN), F32),
            pltpu.VMEM((n, 8, 128), F32),
            pltpu.VMEM((2, 2, rows, dim), BF),
            pltpu.VMEM((3 * width, piece), F32),
            pltpu.VMEM((width, piece), F32),
            pltpu.VMEM((1, piece), F32),
            dma((4,)),
            dma((2, nblk)),
            dma((2, 2)),
            dma((3,)),
            dma((n - 1,)),
            dma((n - 1,)),
            dma((2, n - 1)),
            dma((2, n - 1)),
            dma((2, n - 1)),
            dma((2, n - 1)),
            dma((5, n - 1)),
            dma((5, n - 1)),
            dma((half,)),
            dma((half,)),
            dma((half - 1,)),
            dma((half - 1,)),
            dma((n - 1,)),
            dma((n - 1,)),
        ],
        compiler_params=pltpu.CompilerParams(
            collective_id=1, has_side_effects=True, vmem_limit_bytes=60 * 1024 * 1024
        ),
        name="layer",
    )(
        hist_len,
        states.reshape(total, dim),
        cotangent.reshape(total, dim),
        norm_gain.reshape(1, dim),
        wqkv,
        wout,
    )
    return (
        att.reshape(states.shape),
        gst.reshape(states.shape),
        gq.reshape(3, heads, size, piece).transpose(3, 0, 1, 2),
        go.reshape(heads, size, piece),
        gg.reshape(piece),
    )


def solution(mesh):
    placed = (
        P("dp", None, None),
        P("dp"),
        P(),
        P(None, None, "mp", None),
        P("mp", None, None),
        P("dp", None, None),
    )
    return jax.shard_map(
        functools.partial(body, mesh.shape["dp"], mesh.shape["mp"]),
        mesh=mesh,
        in_specs=placed,
        out_specs=(
            P("dp", None, None),
            P("dp", None, None),
            P("dp", None, "mp", None),
            P("mp", None, "dp"),
            P("dp"),
        ),
        check_vma=False,
    )
```

```python
import functools

import jax
import jax.numpy as jnp
from jax import lax
from jax.experimental import pallas as pl
from jax.experimental.pallas import tpu as pltpu
from jax.sharding import PartitionSpec as P

LEVELS = 4
NB = 4
WIN = 256
PLAN = (
    ((0, 2), "a", 1, 0),
    ((0, 3), "a", 1, 1),
    (("g", 1), "b", 1, 0),
    (("g", 3), "b", 1, 1),
    (("s", 1), "c", 1, 0),
    (("s", 1), "c", 1, 1),
    (("s", 1), "a", 2, 0),
    (("s", 1), "d", 1),
    ((1, 0), "a", 2, 1),
    ((1, 2), "b", 2, 0),
    ((1, 3), "b", 2, 1),
    ((1, 3), "a", 3, 0),
    ((1, 3), "a", 3, 1),
    (("s", 2), "c", 2, 0),
    (("s", 2), "c", 2, 1),
    (("s", 2), "d", 2),
    ((2, 1), "b", 3, 0),
    ((2, 2), "b", 3, 1),
    ((2, 3), "c", 3, 0),
    ((2, 3), "chip"),
    (("s", 3), "c", 3, 1),
    (("s", 3), "d", 3),
    ((4, 1), "sum"),
    (("s", 5), "gain"),
)
BF = jnp.bfloat16
F32 = jnp.float32
MESH = pl.DeviceIdType.MESH


def dot(a, b, ca, cb):
    return lax.dot_general(a, b, (((ca,), (cb,)), ((), ())), preferred_element_type=F32)


def kernel(n, nd, s, hist, states, cot, gain, wqkv, wout, att, gst, gq, go, gg,
           wall, st, mc, normed, inv, pj, sq, sg, scb, gpb, pbb, dsb, ctx, gproj,
           part, got, total, held, tot, zz, res, gqv, gov, ggv,
           s_w, s_in, s_out, s_res, s_z, r_z, s_x, r_x, s_d, r_d, s_c, r_c, s_p, r_p, s_o, r_o, s_g, r_g):
    rows_all, dim = st.shape
    width = wout.shape[0]
    rows = NB * s
    nblk = rows_all // rows
    half = nd // 2
    piece = dim // nd
    d, z = lax.axis_index("dp"), lax.axis_index("mp")
    c, chip = d % 2, d // 2
    bx, by = chip % 2, (chip // 2) % 2
    partner = (d + 1 - 2 * c, z)
    across = ((d + 2 - 4 * bx, z), (d + 4 - 8 * by, z))
    others = [(((chip + o) % half) * 2 + c, z) for o in range(1, half)]
    near = [sorted((abs(k - m), -abs(2 * k + 1 - n), k) for k in range(n) if k != m) for m in range(n)]
    near = [[one[-1] for one in row] for row in near]
    away = [row[:1] + row[:0:-1] if m in (0, n - 1) else row for m, row in enumerate(near)]

    def lookup(table):
        value = table[0]
        for k in range(1, n):
            value = jnp.where(z == k, table[k], value)
        return value

    peer = [None] + [lookup([near[k][m] for k in range(n)]) for m in range(n - 1)]
    goal = [None] + [lookup([away[k][m] for k in range(n)]) for m in range(n - 1)]
    seat = [None] + [lookup([near[away[k][m]].index(k) + 1 for k in range(n)]) for m in range(n - 1)]
    zpeers = [None] + [(d, goal[j]) for j in range(1, n)]

    barrier = pltpu.get_barrier_semaphore()
    greet = zpeers[1:] + others + [partner]
    for device in greet:
        pl.semaphore_signal(barrier, inc=1, device_id=device, device_id_type=MESH)
    loads = []
    for k in range(3):
        loads.append(pltpu.make_async_copy(
            wqkv.at[pl.ds(k * width, width)], wall.at[pl.ds(k * dim, width)], s_w.at[k]))
    loads.append(pltpu.make_async_copy(wout, wall.at[pl.ds(3 * dim, width)], s_w.at[3]))
    for copy in loads:
        copy.start()
    for i in range(nblk):
        at = pl.ds(i * rows, rows)
        pltpu.make_async_copy(states.at[at], st.at[at], s_in.at[0, i]).start()
        pltpu.make_async_copy(cot.at[at], mc.at[at], s_in.at[1, i]).start()

    pj[...] = jnp.zeros_like(pj)
    sq[...] = jnp.zeros_like(sq)
    sg[...] = jnp.zeros_like(sg)
    for copy in loads:
        copy.wait()

    def remote(src, dst, ssem, rsem, device):
        return pltpu.make_async_remote_copy(
            src_ref=src, dst_ref=dst, send_sem=ssem, recv_sem=rsem, device_id=device, device_id_type=MESH
        )

    def arrived(spot, rsem):
        remote(spot, spot, rsem, rsem, partner).wait_recv()

    quarter = width // 4

    def spot(j, x, y, core, i):
        first = pl.multiple_of((x + 2 * y) * dim + j * width + (2 * core + i) * quarter, 16)
        return wall.at[pl.ds(first, quarter)]


    def send_own():
        for j in range(1, n):
            for e in range(2):
                remote(spot(0, bx, by, c, e), spot(seat[j], bx, by, c, e),
                       s_z.at[j - 1, e], r_z.at[seat[j] - 1, e], zpeers[j]).start()

    def first_hop(j, e):
        here = spot(j, bx, by, c, e)
        arrived(here, r_z.at[j - 1, e])
        for i in range(2):
            remote(here, here, s_x.at[i, j - 1, e], r_x.at[i, j - 1, e], across[i]).start()
        remote(here, here, s_c.at[0, j - 1, e], r_c.at[0, j - 1, e], partner).start()

    sides = ((1 - bx, by), (bx, 1 - by))
    diag = (1 - bx, 1 - by)

    def second_hop(j, e):
        for i in (e, 1 - e):
            here = spot(j, *sides[i], c, e)
            arrived(here, r_x.at[i, j - 1, e])
            if i == e:
                remote(here, here, s_d.at[j - 1, e], r_d.at[j - 1, e], across[1 - i]).start()
            remote(here, here, s_c.at[1 + i, j - 1, e], r_c.at[1 + i, j - 1, e], partner).start()

    def third_hop(j, e):
        here = spot(j, *diag, c, e)
        arrived(here, r_d.at[j - 1, e])
        remote(here, here, s_c.at[3, j - 1, e], r_c.at[3, j - 1, e], partner).start()

    def landed(j):
        for e in range(2):
            for k, (x, y) in enumerate(((bx, by),) + sides + (diag,)):
                arrived(spot(j, x, y, 1 - c, e), r_c.at[k, j - 1, e])

    scatter_order = list(range(1, half)) + [0]

    def scatter_core():
        for o in scatter_order:
            t = (chip + o) % half
            remote(part.at[1 - c, t], got.at[o], s_p.at[o], r_p.at[o], partner).start()

    def scatter_chip():
        for o in scatter_order:
            t = (chip + o) % half
            arrived(got.at[o], r_p.at[o])
            both = part[c, t].astype(F32) + got[o].astype(F32)
            if o == 0:
                tot[:piece, :] = both
            else:
                total[o - 1] = both.astype(BF)
                remote(total.at[o - 1], held.at[o - 1], s_o.at[o - 1], r_o.at[o - 1], others[o - 1]).start()

    def scatter_sum():
        for o in range(1, half):
            arrived(held.at[o - 1], r_o.at[o - 1])
            tot[:piece, :] += held[o - 1].astype(F32)
        column = lax.broadcasted_iota(jnp.int32, (dim, 128), 1)
        row = lax.broadcasted_iota(jnp.int32, (dim, 128), 0)
        pick = (row - piece * d == column).astype(F32).astype(BF)
        gsum = jnp.zeros((1, 128), F32)
        for k in range(4):
            m = 4 + k // 2
            turned = jnp.concatenate(
                [tot[:, k * 128 : (k + 1) * 128].T, tot[:, m * 128 : (m + 1) * 128].T[64 * (k % 2) : 64 * (k % 2) + 64]], axis=0
            )
            if k < 3:
                gqv[k * width : (k + 1) * width, :] = turned[:, :piece]
                mine = dot(wall[k * dim : k * dim + width, :], pick, 1, 0)
                gsum = gsum + jnp.sum(mine * turned, axis=0, keepdims=True)
            else:
                gov[...] = turned[:, :piece]
        scale = gain[...].reshape(1, dim)
        own_gain = jnp.ones((1, piece), F32)
        for t in range(nd):
            own_gain = jnp.where(d == t, scale[:, t * piece : (t + 1) * piece], own_gain)
        zz[z, 0:1, :piece] = gsum[:, :piece] / own_gain
        for j in range(1, n):
            remote(zz.at[z], zz.at[z], s_g.at[j - 1], r_g.at[seat[j] - 1], zpeers[j]).start()
        pltpu.make_async_copy(gqv, gq, s_res.at[0]).start()
        pltpu.make_async_copy(gov, go, s_res.at[1]).start()

    def gain_sum():
        for j in range(1, n):
            arrived(zz.at[peer[j]], r_g.at[j - 1])
        value = zz[0, 0:1, :piece]
        for k in range(1, n):
            value = value + zz[k, 0:1, :piece]
        ggv[...] = value
        pltpu.make_async_copy(ggv, gg, s_res.at[2]).start()

    lane = lax.broadcasted_iota(jnp.int32, (s, 128), 1)
    low = (lane < 64).astype(F32).astype(BF)
    high = (lane >= 64).astype(F32).astype(BF)
    key_pos = lax.broadcasted_iota(jnp.int32, (s, WIN), 0)

    def spread(x, out, odd):
        left, right = x[:, :128], x[:, 128:]
        if odd:
            out[0:s, :128] = left * high
            out[s : 2 * s, 128:] = right * low
            out[2 * s : 3 * s, 128:] = right * high
        else:
            out[0:s, :128] = left * low
            out[s : 2 * s, :128] = left * high
            out[2 * s : 3 * s, 128:] = right * low

    def fold(x, odd):
        a, b, e = x[:s], x[s : 2 * s], x[2 * s : 3 * s]
        if odd:
            left = jnp.where(lane < 64, 0.0, a[:, :128])
            right = jnp.where(lane < 64, b[:, 128:], e[:, 128:])
        else:
            left = jnp.where(lane < 64, a[:, :128], b[:, :128])
            right = jnp.where(lane < 64, e[:, 128:], 0.0)
        return jnp.concatenate([left, right], axis=1)

    def put(ref, at, base, x, odd):
        x = x.astype(BF)
        if odd:
            ref[at, base + 128 : base + 256] += x[:, :128]
            ref[at, base + 256 : base + 384] = x[:, 128:]
        else:
            ref[at, base : base + 256] = x

    def prepare(i):
        def fresh():
            at = pl.ds(pl.multiple_of(i * rows, 16), rows)
            pltpu.make_async_copy(states.at[at], st.at[at], s_in.at[0, i]).wait()
            pltpu.make_async_copy(cot.at[at], mc.at[at], s_in.at[1, i]).wait()

        if isinstance(i, int):
            fresh()
        else:
            pl.when(i < nblk)(fresh)
            i = i % nblk
        at = pl.ds(pl.multiple_of(i * rows, 16), rows)
        wide = st[at, :].astype(F32)
        scale = lax.rsqrt(jnp.mean(wide * wide, axis=-1, keepdims=True) + 1e-06)
        inv[at, :] = scale
        normed[at, :] = (wide * scale * gain[...].reshape(1, dim)).astype(BF)
        pos = lax.broadcasted_iota(jnp.int32, (s, dim), 0)
        for b in range(NB):
            one = pl.ds(pl.multiple_of(i * rows + b * s, 16), s)
            keep = pos < LEVELS * hist[i * NB + b]
            mc[one, :] = jnp.where(keep, mc[one, :].astype(F32), 0.0).astype(BF)

    def attention(slot, i):
        odd = slot % 2
        base = 2 * width * (slot // 2)
        first = slot * width - 64 * odd
        cols = width + 64 * odd
        at = pl.ds(pl.multiple_of(i * rows, 16), rows)
        for k in range(4):
            lhs = normed[at, :] if k < 3 else mc[at, :]
            pj[k, :, :cols] = dot(lhs, wall[k * dim + first : k * dim + first + cols, :], 1, 1).astype(BF)

        def scores(b):
            mine = slice(b * s, (b + 1) * s)
            spread(pj[0, mine, :], sq.at[odd, b], odd)
            spread(pj[3, mine, :], sg.at[odd, b], odd)
            scb[b] = dot(pj[1, mine, :], sq[odd, b], 1, 1)
            gpb[b] = dot(pj[2, mine, :], sg[odd, b], 1, 1)

        def soft(b):
            keep = key_pos < LEVELS * hist[i * NB + b]
            sc = jnp.where(keep, scb[b], -1e30)
            ex = jnp.exp(sc - jnp.max(sc, axis=0, keepdims=True))
            prob = ex * (1.0 / jnp.sum(ex, axis=0, keepdims=True))
            pbb[b] = prob.astype(BF)
            gp = gpb[b]
            delta = jnp.sum(prob * gp, axis=0, keepdims=True)
            dsb[b] = (prob * (gp - delta)).astype(BF)

        def outs(b):
            mine = slice(b * s, (b + 1) * s)
            one = pl.ds(pl.multiple_of(i * rows + b * s, 16), s)
            pb, ds = pbb[b], dsb[b]
            put(gproj, one, dim + base, dot(ds, sq[odd, b], 1, 0), odd)
            put(gproj, one, 2 * dim + base, dot(pb, sg[odd, b], 1, 0), odd)
            put(ctx, one, base, fold(dot(pb, pj[2, mine, :], 0, 0), odd), odd)
            put(gproj, one, base, fold(dot(ds, pj[1, mine, :], 0, 0), odd), odd)

        scores(0)
        scores(1)
        for b in range(NB):
            soft(b)
            if b + 2 < NB:
                scores(b + 2)
            outs(b)

    def weight_grads(run):
        kept = None
        for k in range(4):
            run(("g", k))
            lhs = normed[...] if k < 3 else mc[...]
            rhs = gproj[:, k * dim : k * dim + WIN] if k < 3 else ctx[:, :WIN]
            acc = dot(lhs, rhs, 0, 0)
            if k % 2:
                both = kept + pltpu.roll(acc[:, 128:], 64, 1)
            for t in range(nd):
                here = slice(t * piece, (t + 1) * piece)
                part[t % 2, t // 2, :, k * 128 : (k + 1) * 128] = acc[here, :128].astype(BF)
                if k % 2:
                    m = 4 + k // 2
                    part[t % 2, t // 2, :, m * 128 : (m + 1) * 128] = both[here].astype(BF)
            kept = acc[:, 128:]

    def results(i):
        at = pl.ds(pl.multiple_of(i * rows, 16), rows)
        wide = st[at, :].astype(F32)
        copies = [
            pltpu.make_async_copy(res.at[k, i % 2], (att, gst)[k].at[at], s_out.at[k, i % 2]) for k in range(2)
        ]

        @pl.when(i >= 2)
        def _():
            for copy in copies:
                copy.wait()

        res[0, i % 2] = (wide + dot(ctx[at, :], wall[3 * dim :, :], 1, 0)).astype(BF)
        gn = dot(gproj[at, :], wall[: 3 * dim, :], 1, 0)
        scale = inv[at, :]
        unit = wide * scale
        gu = gn * gain[...].reshape(1, dim)
        corr = jnp.mean(gu * unit, axis=-1, keepdims=True)
        res[1, i % 2] = (mc[at, :].astype(F32) + scale * (gu - unit * corr)).astype(BF)
        for copy in copies:
            copy.start()

    def at_step(i, steps):
        for k, step in enumerate(steps):
            if step:
                @pl.when(i == k)
                def _():
                    for one in step:
                        one()

    plan = {}

    def note(when, step, *args):
        plan.setdefault(when, []).append(functools.partial(step, *args))

    for when, step, *args in PLAN:
        note(when, {"a": first_hop, "b": second_hop, "c": third_hop, "d": landed, "chip": scatter_chip,
                    "sum": scatter_sum, "gain": gain_sum}[step], *args)

    def steps(kind):
        return [plan.get((kind, i), ()) for i in range(nblk)]

    def run(when):
        for one in plan.get(when, ()):
            one()

    prepare(0)
    pl.semaphore_wait(barrier, len(greet))
    send_own()
    for m in range(n):
        run(("s", m))

        @pl.loop(0, nblk)
        def _(i):
            at_step(i, steps(m))
            if m == 0:
                prepare(i + 1)
            attention(m, i)

        if m == 0:
            weight_grads(run)
            scatter_core()

    run(("s", n))

    @pl.loop(0, nblk)
    def _(i):
        at_step(i, steps(n))
        results(i)

    run(("s", n + 1))

    for i in range(max(nblk - 2, 0), nblk):
        at = pl.ds(i * rows, rows)
        for k in range(2):
            pltpu.make_async_copy(res.at[k, i % 2], (att, gst)[k].at[at], s_out.at[k, i % 2]).wait()
    pltpu.make_async_copy(gqv, gq, s_res.at[0]).wait()
    pltpu.make_async_copy(gov, go, s_res.at[1]).wait()
    pltpu.make_async_copy(ggv, gg, s_res.at[2]).wait()

    def sent(src, ssem):
        remote(src, src, ssem, ssem, partner).wait_send()

    for j in range(1, n):
        for e in range(2):
            here = spot(j, bx, by, c, e)
            for sem in [s_z.at[j - 1, e], s_d.at[j - 1, e]]:
                sent(here, sem)
            for i in range(2):
                sent(here, s_x.at[i, j - 1, e])
            for k in range(4):
                sent(here, s_c.at[k, j - 1, e])
        sent(zz.at[0], s_g.at[j - 1])
    for o in range(half):
        sent(got.at[o], s_p.at[o])
    for o in range(1, half):
        sent(held.at[o - 1], s_o.at[o - 1])


def settle_kernel(count, *refs):
    srcs, dsts, (big, *small), (sem_in, sem_out) = refs[:5], refs[5:10], refs[10:14], refs[14:]
    rows = big.shape[2]
    ins, outs = [], []
    for i in range(count):
        for k in range(2):
            at = pl.ds(i * rows, rows)
            ins.append(pltpu.make_async_copy(srcs[k].at[at], big.at[k, i], sem_in.at[len(ins)]))
            outs.append(pltpu.make_async_copy(big.at[k, i], dsts[k].at[at], sem_out.at[len(outs)]))
    for k in range(3):
        ins.append(pltpu.make_async_copy(srcs[2 + k], small[k], sem_in.at[len(ins)]))
        outs.append(pltpu.make_async_copy(small[k], dsts[2 + k], sem_out.at[len(outs)]))
    for copy in ins:
        copy.start()
    for one, other in zip(ins, outs):
        one.wait()
        other.start()
    for copy in outs:
        copy.wait()


def settle(arrays):
    count = 4
    rows, dim = arrays[0].shape
    anywhere = pl.BlockSpec(memory_space=pl.ANY)
    return pl.pallas_call(
        functools.partial(settle_kernel, count),
        out_shape=tuple(jax.ShapeDtypeStruct(a.shape, a.dtype) for a in arrays),
        in_specs=(anywhere,) * 5,
        out_specs=(anywhere,) * 5,
        scratch_shapes=[pltpu.VMEM((2, count, rows // count, dim), BF)]
        + [pltpu.VMEM(a.shape, a.dtype) for a in arrays[2:]]
        + [pltpu.SemaphoreType.DMA((2 * count + 3,))] * 2,
        compiler_params=pltpu.CompilerParams(vmem_limit_bytes=60 * 1024 * 1024),
        name="settle",
    )(*arrays)


def body(nd, n, states, hist_len, norm_gain, qkv_weight, output_weight, cotangent):
    dim, _, heads, size = qkv_weight.shape
    count, s, _ = states.shape
    width = heads * size
    total = count * s
    rows = NB * s
    nblk = count // NB
    half = nd // 2
    piece = dim // nd
    wqkv = qkv_weight.transpose(1, 2, 3, 0).reshape(3 * width, dim)
    wout = output_weight.reshape(width, dim)
    anywhere = pl.BlockSpec(memory_space=pl.ANY)
    dma = pltpu.SemaphoreType.DMA
    att, gst, gq, go, gg = pl.pallas_call(
        functools.partial(kernel, n, nd, s),
        out_shape=(
            jax.ShapeDtypeStruct((total, dim), BF),
            jax.ShapeDtypeStruct((total, dim), BF),
            jax.ShapeDtypeStruct((3 * width, piece), F32),
            jax.ShapeDtypeStruct((width, piece), F32),
            jax.ShapeDtypeStruct((1, piece), F32),
        ),
        in_specs=[
            pl.BlockSpec(memory_space=pltpu.SMEM),
            anywhere,
            anywhere,
            pl.BlockSpec(memory_space=pltpu.VMEM),
            anywhere,
            anywhere,
        ],
        out_specs=(anywhere,) * 5,
        scratch_shapes=[
            pltpu.VMEM((4 * dim, dim), BF),
            pltpu.VMEM((total, dim), BF),
            pltpu.VMEM((total, dim), BF),
            pltpu.VMEM((total, dim), BF),
            pltpu.VMEM((total, 1), F32),
            pltpu.VMEM((4, rows, WIN), BF),
            pltpu.VMEM((2, NB, WIN, WIN), BF),
            pltpu.VMEM((2, NB, WIN, WIN), BF),
            pltpu.VMEM((NB, s, WIN), F32),
            pltpu.VMEM((NB, s, WIN), F32),
            pltpu.VMEM((NB, s, WIN), BF),
            pltpu.VMEM((NB, s, WIN), BF),
            pltpu.VMEM((total, dim), BF),
            pltpu.VMEM((total, 3 * dim), BF),
            pltpu.VMEM((2, half, piece, dim), BF),
            pltpu.VMEM((half, piece, dim), BF),
            pltpu.VMEM((half - 1, piece, dim), BF),
            pltpu.VMEM((half - 1, piece, dim), BF),
            pltpu.VMEM((128, dim), F32),
            pltpu.VMEM((n, 8, 128), F32),
            pltpu.VMEM((2, 2, rows, dim), BF),
            pltpu.VMEM((3 * width, piece), F32),
            pltpu.VMEM((width, piece), F32),
            pltpu.VMEM((1, piece), F32),
            dma((4,)),
            dma((2, nblk)),
            dma((2, 2)),
            dma((3,)),
            dma((n - 1, 2)),
            dma((n - 1, 2)),
            dma((2, n - 1, 2)),
            dma((2, n - 1, 2)),
            dma((n - 1, 2)),
            dma((n - 1, 2)),
            dma((4, n - 1, 2)),
            dma((4, n - 1, 2)),
            dma((half,)),
            dma((half,)),
            dma((half - 1,)),
            dma((half - 1,)),
            dma((n - 1,)),
            dma((n - 1,)),
        ],
        compiler_params=pltpu.CompilerParams(
            collective_id=1, has_side_effects=True, vmem_limit_bytes=60 * 1024 * 1024
        ),
        name="layer",
    )(
        hist_len,
        states.reshape(total, dim),
        cotangent.reshape(total, dim),
        norm_gain,
        wqkv,
        wout,
    )
    att, gst, gq, go, gg = settle((att, gst, gq, go, gg))
    return (
        att.reshape(states.shape),
        gst.reshape(states.shape),
        gq.reshape(3, heads, size, piece).transpose(3, 0, 1, 2),
        go.reshape(heads, size, piece),
        gg.reshape(piece),
    )


def solution(mesh):
    placed = (
        P("dp", None, None),
        P("dp"),
        P(),
        P(None, None, "mp", None),
        P("mp", None, None),
        P("dp", None, None),
    )
    return jax.shard_map(
        functools.partial(body, mesh.shape["dp"], mesh.shape["mp"]),
        mesh=mesh,
        in_specs=placed,
        out_specs=(
            P("dp", None, None),
            P("dp", None, None),
            P("dp", None, "mp", None),
            P("mp", None, "dp"),
            P("dp"),
        ),
        check_vma=False,
    )
```

```python
import functools

import jax
import jax.numpy as jnp
from jax import lax
from jax.experimental import pallas as pl
from jax.experimental.pallas import tpu as pltpu
from jax.sharding import PartitionSpec as P

LEVELS = 4
NB = 8
WIN = 256
CHUNK = 32
PLAN = (
    ((0, 1), "z", 1, 0),
    ((0, 1), "a", 1, 0),
    ((0, 1), "in-z", 2, 0),
    (((0, "mid"), 1), "z", 1, 1),
    (((0, "mid"), 1), "a", 1, 1),
    (((0, "mid"), 1), "in-z", 2, 1),
    (("g", 2), "b", 1, 0),
    (("g", 2), "out-z", 2, 0),
    (("g", 2), "in-z", 3, 0),
    (("s", 1), "b", 1, 1),
    (("g", 2), "a", 2, 0),
    (("s", 1), "out-z", 2, 1),
    (("s", 1), "in-z", 3, 1),
    (("s", 1), "a", 2, 1),
    (("s", 1), "c", 1, 0),
    (("s", 1), "c", 1, 1),
    (("s", 1), "d", 1),
    ((1, 0), "b", 2, 0),
    (((1, "mid"), 0), "out-z", 3, 0),
    (((1, "mid"), 0), "b", 2, 1),
    (((1, "mid"), 0), "a", 3, 0),
    ((1, 1), "out-z", 3, 1),
    ((1, 1), "a", 3, 1),
    (((1, "mid"), 1), "c", 2, 0),
    (("s", 2), "c", 2, 1),
    (("s", 2), "d", 2),
    (((2, "mid"), 0), "b", 3, 0),
    ((2, 1), "b", 3, 1),
    (("p", 1), "chip"),
    (("p", 0), "c", 3, 0),
    (("p", 1), "c", 3, 1),
    (("s", 3), "d", 3),
    (("f", 1), "sum"),
    (("s", 5), "gain"),
)
BF = jnp.bfloat16
F32 = jnp.float32
MESH = pl.DeviceIdType.MESH


def dot(a, b, ca, cb):
    return lax.dot_general(a, b, (((ca,), (cb,)), ((), ())), preferred_element_type=F32)


def kernel(n, nd, s, hist, states, cot, gain, wqkv, wout, att, gst, gq, go, gg,
           wall, st, mc, normed, inv, pj, sq, sg, scb, gpb, pbb, dsb, ctx, gproj, ga, aa,
           part, got, total, held, tot, zz, res, gqv, gov, ggv,
           s_w, s_in, s_out, s_res, s_z, s_r, r_z, s_x, r_x, s_d, r_d, s_c, r_c, s_p, r_p, s_o, r_o, s_g, r_g):
    rows_all, dim = st.shape
    width = wout.shape[0]
    rows = NB * s
    nblk = rows_all // rows
    half = nd // 2
    piece = dim // nd
    d, z = lax.axis_index("dp"), lax.axis_index("mp")
    c, chip = d % 2, d // 2
    bx, by = chip % 2, (chip // 2) % 2
    partner = (d + 1 - 2 * c, z)
    across = ((d + 2 - 4 * bx, z), (d + 4 - 8 * by, z))
    others = [(((chip + o) % half) * 2 + c, z) for o in range(1, half)]
    near = [sorted((abs(k - m), -abs(2 * k + 1 - n), k) for k in range(n) if k != m) for m in range(n)]
    near = [[one[-1] for one in row] for row in near]
    away = [row[:1] + row[:0:-1] if m in (0, n - 1) else row for m, row in enumerate(near)]

    def lookup(table):
        value = table[0]
        for k in range(1, n):
            value = jnp.where(z == k, table[k], value)
        return value

    peer = [None] + [lookup([near[k][m] for k in range(n)]) for m in range(n - 1)]
    goal = [None] + [lookup([away[k][m] for k in range(n)]) for m in range(n - 1)]
    seat = [None] + [lookup([near[away[k][m]].index(k) + 1 for k in range(n)]) for m in range(n - 1)]
    zpeers = [None] + [(d, goal[j]) for j in range(1, n)]

    barrier = pltpu.get_barrier_semaphore()
    greet = zpeers[1:] + others + [partner]
    for device in greet:
        pl.semaphore_signal(barrier, inc=1, device_id=device, device_id_type=MESH)
    loads = []
    for k in range(3):
        loads.append(pltpu.make_async_copy(
            wqkv.at[pl.ds(k * width, width)], wall.at[pl.ds(k * dim, width)], s_w.at[k]))
    loads.append(pltpu.make_async_copy(wout, wall.at[pl.ds(3 * dim, width)], s_w.at[3]))
    for copy in loads:
        copy.start()
    for i in range(nblk):
        at = pl.ds(i * rows, rows)
        pltpu.make_async_copy(states.at[at], st.at[at], s_in.at[0, i]).start()
        pltpu.make_async_copy(cot.at[at], mc.at[at], s_in.at[1, i]).start()

    pj[...] = jnp.zeros_like(pj)
    sq[...] = jnp.zeros_like(sq)
    sg[...] = jnp.zeros_like(sg)
    for copy in loads:
        copy.wait()

    def remote(src, dst, ssem, rsem, device):
        return pltpu.make_async_remote_copy(
            src_ref=src, dst_ref=dst, send_sem=ssem, recv_sem=rsem, device_id=device, device_id_type=MESH
        )

    def arrived(spot, rsem):
        remote(spot, spot, rsem, rsem, partner).wait_recv()

    quarter = width // 4

    def spot(j, x, y, core, i):
        first = pl.multiple_of((x + 2 * y) * dim + j * width + (2 * core + i) * quarter, 16)
        return wall.at[pl.ds(first, quarter)]


    inner = jnp.logical_and(z > 0, z < n - 1)
    steps_z = (-1, 1)
    fits = [z > 0, z < n - 1]
    next_z = [(d, (z + n - 1) % n), (d, (z + 1) % n)]

    def seat_at(m, source):
        return near[m].index(source) + 1 if 0 <= m < n else 1

    own_seat = [lookup([seat_at(k + step, k) for k in range(n)]) for step in steps_z]
    onward = [None] + [[lookup([int(near[k][m] * step < k * step and 0 <= k + step < n) for k in range(n)])
                        for step in steps_z] for m in range(n - 1)]
    pass_seat = [None] + [[lookup([seat_at(k + step, near[k][m]) if near[k][m] * step < k * step else 1 for k in range(n)])
                           for step in steps_z] for m in range(n - 1)]

    def send_own():
        for way in range(2):
            @pl.when(fits[way])
            def _():
                for e in range(2):
                    remote(spot(0, bx, by, c, e), spot(own_seat[way], bx, by, c, e),
                           s_z.at[way, e], r_z.at[own_seat[way] - 1, e], next_z[way]).start()

    def relay(j, e):
        here = spot(j, bx, by, c, e)
        arrived(here, r_z.at[j - 1, e])
        for way in range(2):
            @pl.when(onward[j][way] == 1)
            def _():
                remote(here, spot(pass_seat[j][way], bx, by, c, e),
                       s_r.at[j - 1, e], r_z.at[pass_seat[j][way] - 1, e], next_z[way]).start()

    def first_hop(j, e):
        here = spot(j, bx, by, c, e)
        for i in range(2):
            remote(here, here, s_x.at[i, j - 1, e], r_x.at[i, j - 1, e], across[i]).start()
        remote(here, here, s_c.at[0, j - 1, e], r_c.at[0, j - 1, e], partner).start()

    sides = ((1 - bx, by), (bx, 1 - by))
    diag = (1 - bx, 1 - by)

    def second_hop(j, e):
        for i in (e, 1 - e):
            here = spot(j, *sides[i], c, e)
            arrived(here, r_x.at[i, j - 1, e])
            if i == e:
                remote(here, here, s_d.at[j - 1, e], r_d.at[j - 1, e], across[1 - i]).start()
            remote(here, here, s_c.at[1 + i, j - 1, e], r_c.at[1 + i, j - 1, e], partner).start()

    def third_hop(j, e):
        here = spot(j, *diag, c, e)
        arrived(here, r_d.at[j - 1, e])
        remote(here, here, s_c.at[3, j - 1, e], r_c.at[3, j - 1, e], partner).start()

    def landed(j):
        for e in range(2):
            for k, (x, y) in enumerate(((bx, by),) + sides + (diag,)):
                arrived(spot(j, x, y, 1 - c, e), r_c.at[k, j - 1, e])

    scatter_order = list(range(1, half)) + [0]

    def scatter_core():
        for o in scatter_order:
            t = (chip + o) % half
            remote(part.at[1 - c, t], got.at[o], s_p.at[o], r_p.at[o], partner).start()

    def scatter_chip():
        for o in scatter_order:
            t = (chip + o) % half
            arrived(got.at[o], r_p.at[o])
            both = part[c, t].astype(F32) + got[o].astype(F32)
            if o == 0:
                tot[:piece, :] = both
            else:
                total[o - 1] = both.astype(BF)
                remote(total.at[o - 1], held.at[o - 1], s_o.at[o - 1], r_o.at[o - 1], others[o - 1]).start()

    def scatter_sum():
        for o in range(1, half):
            arrived(held.at[o - 1], r_o.at[o - 1])
            tot[:piece, :] += held[o - 1].astype(F32)
        column = lax.broadcasted_iota(jnp.int32, (dim, 128), 1)
        row = lax.broadcasted_iota(jnp.int32, (dim, 128), 0)
        pick = (row - piece * d == column).astype(F32).astype(BF)
        gsum = jnp.zeros((1, 128), F32)
        for k in range(4):
            m = 4 + k // 2
            turned = jnp.concatenate(
                [tot[:, k * 128 : (k + 1) * 128].T, tot[:, m * 128 : (m + 1) * 128].T[64 * (k % 2) : 64 * (k % 2) + 64]], axis=0
            )
            if k < 3:
                gqv[k * width : (k + 1) * width, :] = turned[:, :piece]
                mine = dot(wall[k * dim : k * dim + width, :], pick, 1, 0)
                gsum = gsum + jnp.sum(mine * turned, axis=0, keepdims=True)
            else:
                gov[...] = turned[:, :piece]
        scale = gain[...].reshape(1, dim)
        own_gain = jnp.ones((1, piece), F32)
        for t in range(nd):
            own_gain = jnp.where(d == t, scale[:, t * piece : (t + 1) * piece], own_gain)
        zz[z, 0:1, :piece] = gsum[:, :piece] / own_gain
        for j in range(1, n):
            remote(zz.at[z], zz.at[z], s_g.at[j - 1], r_g.at[seat[j] - 1], zpeers[j]).start()
        pltpu.make_async_copy(gqv, gq, s_res.at[0]).start()
        pltpu.make_async_copy(gov, go, s_res.at[1]).start()

    def gain_sum():
        for j in range(1, n):
            arrived(zz.at[peer[j]], r_g.at[j - 1])
        value = zz[0, 0:1, :piece]
        for k in range(1, n):
            value = value + zz[k, 0:1, :piece]
        ggv[...] = value
        pltpu.make_async_copy(ggv, gg, s_res.at[2]).start()

    lane = lax.broadcasted_iota(jnp.int32, (s, 128), 1)
    low = (lane < 64).astype(F32).astype(BF)
    high = (lane >= 64).astype(F32).astype(BF)
    key_pos = lax.broadcasted_iota(jnp.int32, (s, WIN), 0)

    def spread(x, out, odd):
        left, right = x[:, :128], x[:, 128:]
        if odd:
            out[0:s, :128] = left * high
            out[s : 2 * s, 128:] = right * low
            out[2 * s : 3 * s, 128:] = right * high
        else:
            out[0:s, :128] = left * low
            out[s : 2 * s, :128] = left * high
            out[2 * s : 3 * s, 128:] = right * low

    def fold(x, odd):
        a, b, e = x[:s], x[s : 2 * s], x[2 * s : 3 * s]
        if odd:
            left = jnp.where(lane < 64, 0.0, a[:, :128])
            right = jnp.where(lane < 64, b[:, 128:], e[:, 128:])
        else:
            left = jnp.where(lane < 64, a[:, :128], b[:, :128])
            right = jnp.where(lane < 64, e[:, 128:], 0.0)
        return jnp.concatenate([left, right], axis=1)

    def put(ref, at, base, x, odd):
        x = x.astype(BF)
        if odd:
            ref[at, base + 128 : base + 256] += x[:, :128]
            ref[at, base + 256 : base + 384] = x[:, 128:]
        else:
            ref[at, base : base + 256] = x

    def prepare(i):
        def fresh():
            at = pl.ds(pl.multiple_of(i * rows, 16), rows)
            pltpu.make_async_copy(states.at[at], st.at[at], s_in.at[0, i]).wait()
            pltpu.make_async_copy(cot.at[at], mc.at[at], s_in.at[1, i]).wait()

        if isinstance(i, int):
            fresh()
        else:
            pl.when(i < nblk)(fresh)
            i = i % nblk
        scaled_gain = gain[...].reshape(1, dim)
        for first in range(0, rows, CHUNK):
            some = pl.ds(pl.multiple_of(i * rows + first, 16), CHUNK)
            wide = st[some, :].astype(F32)
            scale = lax.rsqrt(jnp.mean(wide * wide, axis=-1, keepdims=True) + 1e-06)
            inv[some, :] = scale
            normed[some, :] = (wide * scale * scaled_gain).astype(BF)
        pos = lax.broadcasted_iota(jnp.int32, (16, 1), 0)
        for b in range(NB):
            for first in range(0, s, 16):
                some = pl.ds(pl.multiple_of(i * rows + b * s + first, 16), 16)
                keep = (pos + first < LEVELS * hist[i * NB + b]).astype(F32)
                mc[some, :] = jnp.where(keep > 0.0, mc[some, :].astype(F32), 0.0).astype(BF)

    def attention(slot, i):
        odd = slot % 2
        base = 2 * width * (slot // 2)
        first = slot * width - 64 * odd
        cols = width + 64 * odd
        at = pl.ds(pl.multiple_of(i * rows, 16), rows)

        def project(k):
            lhs = normed[at, :] if k < 3 else mc[at, :]
            pj[k, :, :cols] = dot(lhs, wall[k * dim + first : k * dim + first + cols, :], 1, 1).astype(BF)

        def mine(b):
            return slice(b * s, (b + 1) * s)

        def there(b):
            return pl.ds(pl.multiple_of(i * rows + b * s, 16), s)

        def score(b):
            spread(pj[0, mine(b), :], sq.at[odd, b], odd)
            scb[b] = dot(pj[1, mine(b), :], sq[odd, b], 1, 1)

        def soft(b):
            keep = key_pos < LEVELS * hist[i * NB + b]
            sc = jnp.where(keep, scb[b], -1e30)
            ex = jnp.exp(sc - jnp.max(sc, axis=0, keepdims=True))
            prob = ex * (1.0 / jnp.sum(ex, axis=0, keepdims=True))
            scb[b] = prob
            pbb[b] = prob.astype(BF)

        def weigh(b):
            spread(pj[3, mine(b), :], sg.at[odd, b], odd)
            gpb[b] = dot(pj[2, mine(b), :], sg[odd, b], 1, 1)

        def slope(b):
            prob, gp = scb[b], gpb[b]
            delta = jnp.sum(prob * gp, axis=0, keepdims=True)
            dsb[b] = (prob * (gp - delta)).astype(BF)

        def value_grad(b):
            put(gproj, there(b), 2 * dim + base, dot(pbb[b], sg[odd, b], 1, 0), odd)

        def mix(b):
            put(ctx, there(b), base, fold(dot(pbb[b], pj[2, mine(b), :], 0, 0), odd), odd)

        def score_side(b):
            ds = dsb[b]
            put(gproj, there(b), dim + base, dot(ds, sq[odd, b], 1, 0), odd)
            put(gproj, there(b), base, fold(dot(ds, pj[1, mine(b), :], 0, 0), odd), odd)

        every = range(NB)
        for k in range(4):
            project(k)
        at_step(i, steps((slot, "mid")))
        for b in range(NB + 2):
            if b < NB:
                score(b)
                weigh(b)
            if b >= 2:
                value_grad(b - 2)
                mix(b - 2)
                score_side(b - 2)
            if 1 <= b <= NB:
                soft(b - 1)
                slope(b - 1)

    def weight_grads(run):
        kept = None
        for k in range(4):
            if k % 2 == 0:
                run(("g", k))
            lhs = normed[...] if k < 3 else mc[...]
            rhs = gproj[:, k * dim : k * dim + WIN] if k < 3 else ctx[:, :WIN]
            acc = dot(lhs, rhs, 0, 0)
            if k % 2:
                both = kept + pltpu.roll(acc[:, 128:], 64, 1)
            for t in range(nd):
                here = slice(t * piece, (t + 1) * piece)
                part[t % 2, t // 2, :, k * 128 : (k + 1) * 128] = acc[here, :128].astype(BF)
                if k % 2:
                    m = 4 + k // 2
                    part[t % 2, t // 2, :, m * 128 : (m + 1) * 128] = both[here].astype(BF)
            kept = acc[:, 128:]

    early = dim - WIN

    def gather_terms(at, low, high):
        gn = None
        for k in range(3):
            term = dot(gproj[at, k * dim + low : k * dim + high], wall[k * dim + low : k * dim + high, :], 1, 0)
            gn = term if gn is None else gn + term
        return gn, dot(ctx[at, low:high], wall[3 * dim + low : 3 * dim + high, :], 1, 0)

    def partial(i):
        at = pl.ds(pl.multiple_of(i * rows, 16), rows)
        ga[at, :], aa[at, :] = gather_terms(at, 0, early)

    def rest(i):
        at = pl.ds(pl.multiple_of(i * rows, 16), rows)
        gn, mixed = gather_terms(at, early, dim)
        ga[at, :] += gn
        aa[at, :] += mixed

    def finish(i):
        at = pl.ds(pl.multiple_of(i * rows, 16), rows)
        copies = [
            pltpu.make_async_copy(res.at[k, i % 2], (att, gst)[k].at[at], s_out.at[k, i % 2]) for k in range(2)
        ]
        if isinstance(i, int):
            for copy in copies if i >= 2 else ():
                copy.wait()
        else:
            @pl.when(i >= 2)
            def _():
                for copy in copies:
                    copy.wait()

        scaled_gain = gain[...].reshape(1, dim)
        for first in range(0, rows, CHUNK):
            some = pl.ds(pl.multiple_of(i * rows + first, 16), CHUNK)
            wide = st[some, :].astype(F32)
            res[0, i % 2, first : first + CHUNK] = (wide + aa[some, :]).astype(BF)
            scale = inv[some, :]
            unit = wide * scale
            gu = ga[some, :] * scaled_gain
            corr = jnp.mean(gu * unit, axis=-1, keepdims=True)
            res[1, i % 2, first : first + CHUNK] = (mc[some, :].astype(F32) + scale * (gu - unit * corr)).astype(BF)
        return copies

    def at_step(i, steps):
        for k, step in enumerate(steps):
            if step:
                @pl.when(i == k)
                def _():
                    for one in step:
                        one()

    plan = {}

    def note(when, step, *args):
        plan.setdefault(when, []).append(functools.partial(step, *args))

    def only(side, step):
        def run_it(*args):
            pl.when(inner if side == "in" else jnp.logical_not(inner))(functools.partial(step, *args))
        return run_it

    for when, step, *args in PLAN:
        where, _, step = step.rpartition("-")
        action = {"z": relay, "a": first_hop, "b": second_hop, "c": third_hop, "d": landed, "chip": scatter_chip,
                    "sum": scatter_sum, "gain": gain_sum}[step]
        note(when, only(where, action) if where else action, *args)

    def steps(kind):
        return [plan.get((kind, i), ()) for i in range(nblk)]

    def run(when):
        for one in plan.get(when, ()):
            one()

    prepare(0)
    pl.semaphore_wait(barrier, len(greet))
    send_own()
    for m in range(n):
        if m == n - 1:
            @pl.loop(0, nblk)
            def _(i):
                at_step(i, steps("p"))
                partial(i)

        run(("s", m))

        @pl.loop(0, nblk)
        def _(i):
            at_step(i, steps(m))
            if m == 0:
                prepare(i + 1)
            attention(m, i)

        if m == 0:
            weight_grads(run)
            scatter_core()

    run(("s", n))
    rest(0)

    @pl.loop(1, nblk)
    def _(i):
        at_step(i, steps("f"))
        copies = finish(i - 1)
        rest(i)
        for copy in copies:
            copy.start()

    for copy in finish(nblk - 1):
        copy.start()
    run(("s", n + 1))

    for i in range(max(nblk - 2, 0), nblk):
        at = pl.ds(i * rows, rows)
        for k in range(2):
            pltpu.make_async_copy(res.at[k, i % 2], (att, gst)[k].at[at], s_out.at[k, i % 2]).wait()
    pltpu.make_async_copy(gqv, gq, s_res.at[0]).wait()
    pltpu.make_async_copy(gov, go, s_res.at[1]).wait()
    pltpu.make_async_copy(ggv, gg, s_res.at[2]).wait()

    def sent(src, ssem):
        remote(src, src, ssem, ssem, partner).wait_send()

    for way in range(2):
        @pl.when(fits[way])
        def _():
            for e in range(2):
                sent(spot(0, bx, by, c, e), s_z.at[way, e])
    for j in range(1, n):
        for e in range(2):
            here = spot(j, bx, by, c, e)
            sent(here, s_d.at[j - 1, e])
            for way in range(2):
                @pl.when(onward[j][way] == 1)
                def _():
                    sent(here, s_r.at[j - 1, e])
            for i in range(2):
                sent(here, s_x.at[i, j - 1, e])
            for k in range(4):
                sent(here, s_c.at[k, j - 1, e])
        sent(zz.at[0], s_g.at[j - 1])
    for o in range(half):
        sent(got.at[o], s_p.at[o])
    for o in range(1, half):
        sent(held.at[o - 1], s_o.at[o - 1])


def settle_kernel(count, *refs):
    srcs, dsts, (big, *small), (sem_in, sem_out) = refs[:5], refs[5:10], refs[10:14], refs[14:]
    rows = big.shape[2]
    ins, outs = [], []
    for i in range(count):
        for k in range(2):
            at = pl.ds(i * rows, rows)
            ins.append(pltpu.make_async_copy(srcs[k].at[at], big.at[k, i], sem_in.at[len(ins)]))
            outs.append(pltpu.make_async_copy(big.at[k, i], dsts[k].at[at], sem_out.at[len(outs)]))
    for k in range(3):
        ins.append(pltpu.make_async_copy(srcs[2 + k], small[k], sem_in.at[len(ins)]))
        outs.append(pltpu.make_async_copy(small[k], dsts[2 + k], sem_out.at[len(outs)]))
    for copy in ins:
        copy.start()
    for one, other in zip(ins, outs):
        one.wait()
        other.start()
    for copy in outs:
        copy.wait()


def settle(arrays):
    count = 4
    rows, dim = arrays[0].shape
    anywhere = pl.BlockSpec(memory_space=pl.ANY)
    return pl.pallas_call(
        functools.partial(settle_kernel, count),
        out_shape=tuple(jax.ShapeDtypeStruct(a.shape, a.dtype) for a in arrays),
        in_specs=(anywhere,) * 5,
        out_specs=(anywhere,) * 5,
        scratch_shapes=[pltpu.VMEM((2, count, rows // count, dim), BF)]
        + [pltpu.VMEM(a.shape, a.dtype) for a in arrays[2:]]
        + [pltpu.SemaphoreType.DMA((2 * count + 3,))] * 2,
        compiler_params=pltpu.CompilerParams(vmem_limit_bytes=60 * 1024 * 1024),
        name="settle",
    )(*arrays)


def body(nd, n, states, hist_len, norm_gain, qkv_weight, output_weight, cotangent):
    dim, _, heads, size = qkv_weight.shape
    count, s, _ = states.shape
    width = heads * size
    total = count * s
    rows = NB * s
    nblk = count // NB
    half = nd // 2
    piece = dim // nd
    wqkv = qkv_weight.transpose(1, 2, 3, 0).reshape(3 * width, dim)
    wout = output_weight.reshape(width, dim)
    anywhere = pl.BlockSpec(memory_space=pl.ANY)
    dma = pltpu.SemaphoreType.DMA
    att, gst, gq, go, gg = pl.pallas_call(
        functools.partial(kernel, n, nd, s),
        out_shape=(
            jax.ShapeDtypeStruct((total, dim), BF),
            jax.ShapeDtypeStruct((total, dim), BF),
            jax.ShapeDtypeStruct((3 * width, piece), F32),
            jax.ShapeDtypeStruct((width, piece), F32),
            jax.ShapeDtypeStruct((1, piece), F32),
        ),
        in_specs=[
            pl.BlockSpec(memory_space=pltpu.SMEM),
            anywhere,
            anywhere,
            pl.BlockSpec(memory_space=pltpu.VMEM),
            anywhere,
            anywhere,
        ],
        out_specs=(anywhere,) * 5,
        scratch_shapes=[
            pltpu.VMEM((4 * dim, dim), BF),
            pltpu.VMEM((total, dim), BF),
            pltpu.VMEM((total, dim), BF),
            pltpu.VMEM((total, dim), BF),
            pltpu.VMEM((total, 1), F32),
            pltpu.VMEM((4, rows, WIN), BF),
            pltpu.VMEM((2, NB, WIN, WIN), BF),
            pltpu.VMEM((2, NB, WIN, WIN), BF),
            pltpu.VMEM((NB, s, WIN), F32),
            pltpu.VMEM((NB, s, WIN), F32),
            pltpu.VMEM((NB, s, WIN), BF),
            pltpu.VMEM((NB, s, WIN), BF),
            pltpu.VMEM((total, dim), BF),
            pltpu.VMEM((total, 3 * dim), BF),
            pltpu.VMEM((total, dim), F32),
            pltpu.VMEM((total, dim), F32),
            pltpu.VMEM((2, half, piece, dim), BF),
            pltpu.VMEM((half, piece, dim), BF),
            pltpu.VMEM((half - 1, piece, dim), BF),
            pltpu.VMEM((half - 1, piece, dim), BF),
            pltpu.VMEM((128, dim), F32),
            pltpu.VMEM((n, 8, 128), F32),
            pltpu.VMEM((2, 2, rows, dim), BF),
            pltpu.VMEM((3 * width, piece), F32),
            pltpu.VMEM((width, piece), F32),
            pltpu.VMEM((1, piece), F32),
            dma((4,)),
            dma((2, nblk)),
            dma((2, 2)),
            dma((3,)),
            dma((2, 2)),
            dma((n - 1, 2)),
            dma((n - 1, 2)),
            dma((2, n - 1, 2)),
            dma((2, n - 1, 2)),
            dma((n - 1, 2)),
            dma((n - 1, 2)),
            dma((4, n - 1, 2)),
            dma((4, n - 1, 2)),
            dma((half,)),
            dma((half,)),
            dma((half - 1,)),
            dma((half - 1,)),
            dma((n - 1,)),
            dma((n - 1,)),
        ],
        compiler_params=pltpu.CompilerParams(
            collective_id=1, has_side_effects=True, vmem_limit_bytes=60 * 1024 * 1024
        ),
        name="layer",
    )(
        hist_len,
        states.reshape(total, dim),
        cotangent.reshape(total, dim),
        norm_gain,
        wqkv,
        wout,
    )
    att, gst, gq, go, gg = settle((att, gst, gq, go, gg))
    return (
        att.reshape(states.shape),
        gst.reshape(states.shape),
        gq.reshape(3, heads, size, piece).transpose(3, 0, 1, 2),
        go.reshape(heads, size, piece),
        gg.reshape(piece),
    )


def solution(mesh):
    placed = (
        P("dp", None, None),
        P("dp"),
        P(),
        P(None, None, "mp", None),
        P("mp", None, None),
        P("dp", None, None),
    )
    return jax.shard_map(
        functools.partial(body, mesh.shape["dp"], mesh.shape["mp"]),
        mesh=mesh,
        in_specs=placed,
        out_specs=(
            P("dp", None, None),
            P("dp", None, None),
            P("dp", None, "mp", None),
            P("mp", None, "dp"),
            P("dp"),
        ),
        check_vma=False,
    )
```

```python
import functools

import jax
import jax.numpy as jnp
from jax import lax
from jax.experimental import pallas as pl
from jax.experimental.pallas import tpu as pltpu
from jax.sharding import PartitionSpec as P

LEVELS = 4
NB = 8
WIN = 256
CHUNK = 32
PLAN = (
    ((0, 1), "z", 1, 0),
    ((0, 1), "a", 1, 0),
    ((0, 1), "in-z", 2, 0),
    (((0, "mid"), 1), "z", 1, 1),
    (((0, "mid"), 1), "a", 1, 1),
    (((0, "mid"), 1), "in-z", 2, 1),
    (("g", 2), "b", 1, 0),
    (("g", 2), "out-z", 2, 0),
    (("g", 2), "in-z", 3, 0),
    (("s", 1), "b", 1, 1),
    (("g", 2), "a", 2, 0),
    (("s", 1), "out-z", 2, 1),
    (("s", 1), "in-z", 3, 1),
    (("s", 1), "a", 2, 1),
    (("s", 1), "c", 1, 0),
    (("s", 1), "c", 1, 1),
    (("s", 1), "d", 1),
    ((1, 0), "b", 2, 0),
    (((1, "mid"), 0), "out-z", 3, 0),
    (((1, "mid"), 0), "b", 2, 1),
    (((1, "mid"), 0), "a", 3, 0),
    ((1, 1), "out-z", 3, 1),
    ((1, 1), "a", 3, 1),
    (((1, "mid"), 1), "c", 2, 0),
    (("s", 2), "c", 2, 1),
    (("s", 2), "d", 2),
    (((2, "mid"), 0), "b", 3, 0),
    ((2, 1), "b", 3, 1),
    (("p", 1), "chip"),
    (("p", 0), "c", 3, 0),
    (("p", 1), "c", 3, 1),
    (("s", 3), "d", 3),
    (("s", 4), "sum"),
    (("s", 5), "gain"),
)
BF = jnp.bfloat16
F32 = jnp.float32
MESH = pl.DeviceIdType.MESH


def dot(a, b, ca, cb):
    return lax.dot_general(a, b, (((ca,), (cb,)), ((), ())), preferred_element_type=F32)


def kernel(n, nd, s, hist, states, cot, gain, wqkv, wout, att, gst, gq, go, gg,
           wall, st, mc, normed, inv, pj, sq, sg, scb, gpb, pbb, dsb, ctx, gproj, ga, aa,
           part, got, total, held, tot, zz, res, gqv, gov, ggv,
           s_w, s_in, s_out, s_res, s_z, s_r, r_z, s_x, r_x, s_d, r_d, s_c, r_c, s_p, r_p, s_o, r_o, s_g, r_g):
    rows_all, dim = st.shape
    width = wout.shape[0]
    rows = NB * s
    nblk = rows_all // rows
    half = nd // 2
    piece = dim // nd
    d, z = lax.axis_index("dp"), lax.axis_index("mp")
    c, chip = d % 2, d // 2
    bx, by = chip % 2, (chip // 2) % 2
    partner = (d + 1 - 2 * c, z)
    across = ((d + 2 - 4 * bx, z), (d + 4 - 8 * by, z))
    others = [(((chip + o) % half) * 2 + c, z) for o in range(1, half)]
    near = [sorted((abs(k - m), -abs(2 * k + 1 - n), k) for k in range(n) if k != m) for m in range(n)]
    near = [[one[-1] for one in row] for row in near]
    away = [row[:1] + row[:0:-1] if m in (0, n - 1) else row for m, row in enumerate(near)]

    def lookup(table):
        value = table[0]
        for k in range(1, n):
            value = jnp.where(z == k, table[k], value)
        return value

    peer = [None] + [lookup([near[k][m] for k in range(n)]) for m in range(n - 1)]
    goal = [None] + [lookup([away[k][m] for k in range(n)]) for m in range(n - 1)]
    seat = [None] + [lookup([near[away[k][m]].index(k) + 1 for k in range(n)]) for m in range(n - 1)]
    zpeers = [None] + [(d, goal[j]) for j in range(1, n)]

    barrier = pltpu.get_barrier_semaphore()
    greet = zpeers[1:] + others + [partner]
    for device in greet:
        pl.semaphore_signal(barrier, inc=1, device_id=device, device_id_type=MESH)
    loads = []
    for k in range(3):
        loads.append(pltpu.make_async_copy(
            wqkv.at[pl.ds(k * width, width)], wall.at[pl.ds(k * dim, width)], s_w.at[k]))
    loads.append(pltpu.make_async_copy(wout, wall.at[pl.ds(3 * dim, width)], s_w.at[3]))
    for copy in loads:
        copy.start()
    for i in range(nblk):
        at = pl.ds(i * rows, rows)
        pltpu.make_async_copy(states.at[at], st.at[at], s_in.at[0, i]).start()
        pltpu.make_async_copy(cot.at[at], mc.at[at], s_in.at[1, i]).start()

    pj[...] = jnp.zeros_like(pj)
    sq[...] = jnp.zeros_like(sq)
    sg[...] = jnp.zeros_like(sg)
    for copy in loads:
        copy.wait()

    def remote(src, dst, ssem, rsem, device):
        return pltpu.make_async_remote_copy(
            src_ref=src, dst_ref=dst, send_sem=ssem, recv_sem=rsem, device_id=device, device_id_type=MESH
        )

    def arrived(spot, rsem):
        remote(spot, spot, rsem, rsem, partner).wait_recv()

    quarter = width // 4

    def spot(j, x, y, core, i):
        first = pl.multiple_of((x + 2 * y) * dim + j * width + (2 * core + i) * quarter, 16)
        return wall.at[pl.ds(first, quarter)]


    inner = jnp.logical_and(z > 0, z < n - 1)
    steps_z = (-1, 1)
    fits = [z > 0, z < n - 1]
    next_z = [(d, (z + n - 1) % n), (d, (z + 1) % n)]

    def seat_at(m, source):
        return near[m].index(source) + 1 if 0 <= m < n else 1

    own_seat = [lookup([seat_at(k + step, k) for k in range(n)]) for step in steps_z]
    onward = [None] + [[lookup([int(near[k][m] * step < k * step and 0 <= k + step < n) for k in range(n)])
                        for step in steps_z] for m in range(n - 1)]
    pass_seat = [None] + [[lookup([seat_at(k + step, near[k][m]) if near[k][m] * step < k * step else 1 for k in range(n)])
                           for step in steps_z] for m in range(n - 1)]

    def send_own():
        for way in range(2):
            @pl.when(fits[way])
            def _():
                for e in range(2):
                    remote(spot(0, bx, by, c, e), spot(own_seat[way], bx, by, c, e),
                           s_z.at[way, e], r_z.at[own_seat[way] - 1, e], next_z[way]).start()

    def relay(j, e):
        here = spot(j, bx, by, c, e)
        arrived(here, r_z.at[j - 1, e])
        for way in range(2):
            @pl.when(onward[j][way] == 1)
            def _():
                remote(here, spot(pass_seat[j][way], bx, by, c, e),
                       s_r.at[j - 1, e], r_z.at[pass_seat[j][way] - 1, e], next_z[way]).start()

    def first_hop(j, e):
        here = spot(j, bx, by, c, e)
        for i in range(2):
            remote(here, here, s_x.at[i, j - 1, e], r_x.at[i, j - 1, e], across[i]).start()
        remote(here, here, s_c.at[0, j - 1, e], r_c.at[0, j - 1, e], partner).start()

    sides = ((1 - bx, by), (bx, 1 - by))
    diag = (1 - bx, 1 - by)

    def second_hop(j, e):
        for i in (e, 1 - e):
            here = spot(j, *sides[i], c, e)
            arrived(here, r_x.at[i, j - 1, e])
            if i == e:
                remote(here, here, s_d.at[j - 1, e], r_d.at[j - 1, e], across[1 - i]).start()
            remote(here, here, s_c.at[1 + i, j - 1, e], r_c.at[1 + i, j - 1, e], partner).start()

    def third_hop(j, e):
        here = spot(j, *diag, c, e)
        arrived(here, r_d.at[j - 1, e])
        remote(here, here, s_c.at[3, j - 1, e], r_c.at[3, j - 1, e], partner).start()

    def landed(j):
        for e in range(2):
            for k, (x, y) in enumerate(((bx, by),) + sides + (diag,)):
                arrived(spot(j, x, y, 1 - c, e), r_c.at[k, j - 1, e])

    scatter_order = list(range(1, half)) + [0]

    def scatter_core():
        for o in scatter_order:
            t = (chip + o) % half
            remote(part.at[1 - c, t], got.at[o], s_p.at[o], r_p.at[o], partner).start()

    def scatter_chip():
        for o in scatter_order:
            t = (chip + o) % half
            arrived(got.at[o], r_p.at[o])
            both = part[c, t].astype(F32) + got[o].astype(F32)
            if o == 0:
                tot[:piece, :] = both
            else:
                total[o - 1] = both.astype(BF)
                remote(total.at[o - 1], held.at[o - 1], s_o.at[o - 1], r_o.at[o - 1], others[o - 1]).start()

    def scatter_sum():
        for o in range(1, half):
            arrived(held.at[o - 1], r_o.at[o - 1])
            tot[:piece, :] += held[o - 1].astype(F32)
        column = lax.broadcasted_iota(jnp.int32, (dim, 128), 1)
        row = lax.broadcasted_iota(jnp.int32, (dim, 128), 0)
        pick = (row - piece * d == column).astype(F32).astype(BF)
        gsum = jnp.zeros((1, 128), F32)
        for k in range(4):
            m = 4 + k // 2
            turned = jnp.concatenate(
                [tot[:, k * 128 : (k + 1) * 128].T, tot[:, m * 128 : (m + 1) * 128].T[64 * (k % 2) : 64 * (k % 2) + 64]], axis=0
            )
            if k < 3:
                gqv[k * width : (k + 1) * width, :] = turned[:, :piece]
                mine = dot(wall[k * dim : k * dim + width, :], pick, 1, 0)
                gsum = gsum + jnp.sum(mine * turned, axis=0, keepdims=True)
            else:
                gov[...] = turned[:, :piece]
        scale = gain[...].reshape(1, dim)
        own_gain = jnp.ones((1, piece), F32)
        for t in range(nd):
            own_gain = jnp.where(d == t, scale[:, t * piece : (t + 1) * piece], own_gain)
        zz[z, 0:1, :piece] = gsum[:, :piece] / own_gain
        for j in range(1, n):
            remote(zz.at[z], zz.at[z], s_g.at[j - 1], r_g.at[seat[j] - 1], zpeers[j]).start()
        pltpu.make_async_copy(gqv, gq, s_res.at[0]).start()
        pltpu.make_async_copy(gov, go, s_res.at[1]).start()

    def gain_sum():
        for j in range(1, n):
            arrived(zz.at[peer[j]], r_g.at[j - 1])
        value = zz[0, 0:1, :piece]
        for k in range(1, n):
            value = value + zz[k, 0:1, :piece]
        ggv[...] = value
        pltpu.make_async_copy(ggv, gg, s_res.at[2]).start()

    lane = lax.broadcasted_iota(jnp.int32, (s, 128), 1)
    low = (lane < 64).astype(F32).astype(BF)
    high = (lane >= 64).astype(F32).astype(BF)
    key_pos = lax.broadcasted_iota(jnp.int32, (s, WIN), 0)

    def spread(x, out, odd):
        left, right = x[:, :128], x[:, 128:]
        if odd:
            out[0:s, :128] = left * high
            out[s : 2 * s, 128:] = right * low
            out[2 * s : 3 * s, 128:] = right * high
        else:
            out[0:s, :128] = left * low
            out[s : 2 * s, :128] = left * high
            out[2 * s : 3 * s, 128:] = right * low

    def fold(x, odd):
        a, b, e = x[:s], x[s : 2 * s], x[2 * s : 3 * s]
        if odd:
            left = jnp.where(lane < 64, 0.0, a[:, :128])
            right = jnp.where(lane < 64, b[:, 128:], e[:, 128:])
        else:
            left = jnp.where(lane < 64, a[:, :128], b[:, :128])
            right = jnp.where(lane < 64, e[:, 128:], 0.0)
        return jnp.concatenate([left, right], axis=1)

    def put(ref, at, base, x, odd):
        x = x.astype(BF)
        if odd:
            ref[at, base + 128 : base + 256] += x[:, :128]
            ref[at, base + 256 : base + 384] = x[:, 128:]
        else:
            ref[at, base : base + 256] = x

    def prepare(i):
        def fresh():
            at = pl.ds(pl.multiple_of(i * rows, 16), rows)
            pltpu.make_async_copy(states.at[at], st.at[at], s_in.at[0, i]).wait()
            pltpu.make_async_copy(cot.at[at], mc.at[at], s_in.at[1, i]).wait()

        if isinstance(i, int):
            fresh()
        else:
            pl.when(i < nblk)(fresh)
            i = i % nblk
        scaled_gain = gain[...].reshape(1, dim)
        for first in range(0, rows, CHUNK):
            some = pl.ds(pl.multiple_of(i * rows + first, 16), CHUNK)
            wide = st[some, :].astype(F32)
            scale = lax.rsqrt(jnp.mean(wide * wide, axis=-1, keepdims=True) + 1e-06)
            inv[some, :] = scale
            normed[some, :] = (wide * scale * scaled_gain).astype(BF)
        pos = lax.broadcasted_iota(jnp.int32, (16, 1), 0)
        for b in range(NB):
            for first in range(0, s, 16):
                some = pl.ds(pl.multiple_of(i * rows + b * s + first, 16), 16)
                keep = (pos + first < LEVELS * hist[i * NB + b]).astype(F32)
                mc[some, :] = jnp.where(keep > 0.0, mc[some, :].astype(F32), 0.0).astype(BF)

    def attention(slot, i):
        odd = slot % 2
        base = 2 * width * (slot // 2)
        first = slot * width - 64 * odd
        cols = width + 64 * odd
        at = pl.ds(pl.multiple_of(i * rows, 16), rows)

        def project(k):
            lhs = normed[at, :] if k < 3 else mc[at, :]
            pj[k, :, :cols] = dot(lhs, wall[k * dim + first : k * dim + first + cols, :], 1, 1).astype(BF)

        def mine(b):
            return slice(b * s, (b + 1) * s)

        def there(b):
            return pl.ds(pl.multiple_of(i * rows + b * s, 16), s)

        def score(b):
            spread(pj[0, mine(b), :], sq.at[odd, b], odd)
            scb[b] = dot(pj[1, mine(b), :], sq[odd, b], 1, 1)

        def soft(b):
            keep = key_pos < LEVELS * hist[i * NB + b]
            sc = jnp.where(keep, scb[b], -1e30)
            ex = jnp.exp(sc - jnp.max(sc, axis=0, keepdims=True))
            prob = ex * (1.0 / jnp.sum(ex, axis=0, keepdims=True))
            scb[b] = prob
            pbb[b] = prob.astype(BF)

        def weigh(b):
            spread(pj[3, mine(b), :], sg.at[odd, b], odd)
            gpb[b] = dot(pj[2, mine(b), :], sg[odd, b], 1, 1)

        def slope(b):
            prob, gp = scb[b], gpb[b]
            delta = jnp.sum(prob * gp, axis=0, keepdims=True)
            dsb[b] = (prob * (gp - delta)).astype(BF)

        def value_grad(b):
            put(gproj, there(b), 2 * dim + base, dot(pbb[b], sg[odd, b], 1, 0), odd)

        def mix(b):
            put(ctx, there(b), base, fold(dot(pbb[b], pj[2, mine(b), :], 0, 0), odd), odd)

        def score_side(b):
            ds = dsb[b]
            put(gproj, there(b), dim + base, dot(ds, sq[odd, b], 1, 0), odd)
            put(gproj, there(b), base, fold(dot(ds, pj[1, mine(b), :], 0, 0), odd), odd)

        every = range(NB)
        for k in range(4):
            project(k)
        at_step(i, steps((slot, "mid")))
        for b in range(NB + 2):
            if b < NB:
                score(b)
                weigh(b)
            if b >= 2:
                value_grad(b - 2)
                mix(b - 2)
                score_side(b - 2)
            if 1 <= b <= NB:
                soft(b - 1)
                slope(b - 1)

    def weight_grads(run):
        kept = None
        for k in range(4):
            if k % 2 == 0:
                run(("g", k))
            lhs = normed[...] if k < 3 else mc[...]
            rhs = gproj[:, k * dim : k * dim + WIN] if k < 3 else ctx[:, :WIN]
            acc = dot(lhs, rhs, 0, 0)
            if k % 2:
                both = kept + pltpu.roll(acc[:, 128:], 64, 1)
            for t in range(nd):
                here = slice(t * piece, (t + 1) * piece)
                part[t % 2, t // 2, :, k * 128 : (k + 1) * 128] = acc[here, :128].astype(BF)
                if k % 2:
                    m = 4 + k // 2
                    part[t % 2, t // 2, :, m * 128 : (m + 1) * 128] = both[here].astype(BF)
            kept = acc[:, 128:]

    early = dim - WIN

    def gather_terms(at, low, high):
        gn = None
        for k in range(3):
            term = dot(gproj[at, k * dim + low : k * dim + high], wall[k * dim + low : k * dim + high, :], 1, 0)
            gn = term if gn is None else gn + term
        return gn, dot(ctx[at, low:high], wall[3 * dim + low : 3 * dim + high, :], 1, 0)

    def partial(i):
        at = pl.ds(pl.multiple_of(i * rows, 16), rows)
        ga[at, :], aa[at, :] = gather_terms(at, 0, early)

    def rest(i):
        at = pl.ds(pl.multiple_of(i * rows, 16), rows)
        gn, mixed = gather_terms(at, early, dim)
        ga[at, :] += gn
        aa[at, :] += mixed

    def finish(i):
        at = pl.ds(pl.multiple_of(i * rows, 16), rows)
        copies = [
            pltpu.make_async_copy(res.at[k, i % 2], (att, gst)[k].at[at], s_out.at[k, i % 2]) for k in range(2)
        ]
        if isinstance(i, int):
            for copy in copies if i >= 2 else ():
                copy.wait()
        else:
            @pl.when(i >= 2)
            def _():
                for copy in copies:
                    copy.wait()

        scaled_gain = gain[...].reshape(1, dim)
        for first in range(0, rows, CHUNK):
            some = pl.ds(pl.multiple_of(i * rows + first, 16), CHUNK)
            wide = st[some, :].astype(F32)
            res[0, i % 2, first : first + CHUNK] = (wide + aa[some, :]).astype(BF)
            scale = inv[some, :]
            unit = wide * scale
            gu = ga[some, :] * scaled_gain
            corr = jnp.mean(gu * unit, axis=-1, keepdims=True)
            res[1, i % 2, first : first + CHUNK] = (mc[some, :].astype(F32) + scale * (gu - unit * corr)).astype(BF)
        return copies

    def at_step(i, steps):
        for k, step in enumerate(steps):
            if step:
                @pl.when(i == k)
                def _():
                    for one in step:
                        one()

    plan = {}

    def note(when, step, *args):
        plan.setdefault(when, []).append(functools.partial(step, *args))

    def only(side, step):
        def run_it(*args):
            pl.when(inner if side == "in" else jnp.logical_not(inner))(functools.partial(step, *args))
        return run_it

    for when, step, *args in PLAN:
        where, _, step = step.rpartition("-")
        action = {"z": relay, "a": first_hop, "b": second_hop, "c": third_hop, "d": landed, "chip": scatter_chip,
                    "sum": scatter_sum, "gain": gain_sum}[step]
        note(when, only(where, action) if where else action, *args)

    def steps(kind):
        return [plan.get((kind, i), ()) for i in range(nblk)]

    def run(when):
        for one in plan.get(when, ()):
            one()

    pl.semaphore_wait(barrier, len(greet))
    send_own()
    prepare(0)
    for m in range(n):
        if m == n - 1:
            @pl.loop(0, nblk)
            def _(i):
                at_step(i, steps("p"))
                partial(i)

        run(("s", m))

        @pl.loop(0, nblk)
        def _(i):
            at_step(i, steps(m))
            if m == 0:
                prepare(i + 1)
            attention(m, i)

        if m == 0:
            weight_grads(run)
            scatter_core()

    run(("s", n))
    rest(0)

    @pl.loop(1, nblk)
    def _(i):
        at_step(i, steps("f"))
        copies = finish(i - 1)
        rest(i)
        for copy in copies:
            copy.start()

    for copy in finish(nblk - 1):
        copy.start()
    run(("s", n + 1))

    for i in range(max(nblk - 2, 0), nblk):
        at = pl.ds(i * rows, rows)
        for k in range(2):
            pltpu.make_async_copy(res.at[k, i % 2], (att, gst)[k].at[at], s_out.at[k, i % 2]).wait()
    pltpu.make_async_copy(gqv, gq, s_res.at[0]).wait()
    pltpu.make_async_copy(gov, go, s_res.at[1]).wait()
    pltpu.make_async_copy(ggv, gg, s_res.at[2]).wait()

    def sent(src, ssem):
        remote(src, src, ssem, ssem, partner).wait_send()

    for way in range(2):
        @pl.when(fits[way])
        def _():
            for e in range(2):
                sent(spot(0, bx, by, c, e), s_z.at[way, e])
    for j in range(1, n):
        for e in range(2):
            here = spot(j, bx, by, c, e)
            sent(here, s_d.at[j - 1, e])
            for way in range(2):
                @pl.when(onward[j][way] == 1)
                def _():
                    sent(here, s_r.at[j - 1, e])
            for i in range(2):
                sent(here, s_x.at[i, j - 1, e])
            for k in range(4):
                sent(here, s_c.at[k, j - 1, e])
        sent(zz.at[0], s_g.at[j - 1])
    for o in range(half):
        sent(got.at[o], s_p.at[o])
    for o in range(1, half):
        sent(held.at[o - 1], s_o.at[o - 1])


def settle_kernel(count, *refs):
    srcs, dsts, (big, *small), (sem_in, sem_out) = refs[:5], refs[5:10], refs[10:14], refs[14:]
    rows = big.shape[2]
    ins, outs = [], []
    for i in range(count):
        for k in range(2):
            at = pl.ds(i * rows, rows)
            ins.append(pltpu.make_async_copy(srcs[k].at[at], big.at[k, i], sem_in.at[len(ins)]))
            outs.append(pltpu.make_async_copy(big.at[k, i], dsts[k].at[at], sem_out.at[len(outs)]))
    for k in range(3):
        ins.append(pltpu.make_async_copy(srcs[2 + k], small[k], sem_in.at[len(ins)]))
        outs.append(pltpu.make_async_copy(small[k], dsts[2 + k], sem_out.at[len(outs)]))
    for copy in ins:
        copy.start()
    for one, other in zip(ins, outs):
        one.wait()
        other.start()
    for copy in outs:
        copy.wait()


def settle(arrays):
    count = 8
    rows, dim = arrays[0].shape
    anywhere = pl.BlockSpec(memory_space=pl.ANY)
    return pl.pallas_call(
        functools.partial(settle_kernel, count),
        out_shape=tuple(jax.ShapeDtypeStruct(a.shape, a.dtype) for a in arrays),
        in_specs=(anywhere,) * 5,
        out_specs=(anywhere,) * 5,
        scratch_shapes=[pltpu.VMEM((2, count, rows // count, dim), BF)]
        + [pltpu.VMEM(a.shape, a.dtype) for a in arrays[2:]]
        + [pltpu.SemaphoreType.DMA((2 * count + 3,))] * 2,
        compiler_params=pltpu.CompilerParams(vmem_limit_bytes=60 * 1024 * 1024),
        name="settle",
    )(*arrays)


def body(nd, n, states, hist_len, norm_gain, qkv_weight, output_weight, cotangent):
    dim, _, heads, size = qkv_weight.shape
    count, s, _ = states.shape
    width = heads * size
    total = count * s
    rows = NB * s
    nblk = count // NB
    half = nd // 2
    piece = dim // nd
    wqkv = qkv_weight.transpose(1, 2, 3, 0).reshape(3 * width, dim)
    wout = output_weight.reshape(width, dim)
    anywhere = pl.BlockSpec(memory_space=pl.ANY)
    dma = pltpu.SemaphoreType.DMA
    att, gst, gq, go, gg = pl.pallas_call(
        functools.partial(kernel, n, nd, s),
        out_shape=(
            jax.ShapeDtypeStruct((total, dim), BF),
            jax.ShapeDtypeStruct((total, dim), BF),
            jax.ShapeDtypeStruct((3 * width, piece), F32),
            jax.ShapeDtypeStruct((width, piece), F32),
            jax.ShapeDtypeStruct((1, piece), F32),
        ),
        in_specs=[
            pl.BlockSpec(memory_space=pltpu.SMEM),
            anywhere,
            anywhere,
            pl.BlockSpec(memory_space=pltpu.VMEM),
            anywhere,
            anywhere,
        ],
        out_specs=(anywhere,) * 5,
        scratch_shapes=[
            pltpu.VMEM((4 * dim, dim), BF),
            pltpu.VMEM((total, dim), BF),
            pltpu.VMEM((total, dim), BF),
            pltpu.VMEM((total, dim), BF),
            pltpu.VMEM((total, 1), F32),
            pltpu.VMEM((4, rows, WIN), BF),
            pltpu.VMEM((2, NB, WIN, WIN), BF),
            pltpu.VMEM((2, NB, WIN, WIN), BF),
            pltpu.VMEM((NB, s, WIN), F32),
            pltpu.VMEM((NB, s, WIN), F32),
            pltpu.VMEM((NB, s, WIN), BF),
            pltpu.VMEM((NB, s, WIN), BF),
            pltpu.VMEM((total, dim), BF),
            pltpu.VMEM((total, 3 * dim), BF),
            pltpu.VMEM((total, dim), F32),
            pltpu.VMEM((total, dim), F32),
            pltpu.VMEM((2, half, piece, dim), BF),
            pltpu.VMEM((half, piece, dim), BF),
            pltpu.VMEM((half - 1, piece, dim), BF),
            pltpu.VMEM((half - 1, piece, dim), BF),
            pltpu.VMEM((128, dim), F32),
            pltpu.VMEM((n, 8, 128), F32),
            pltpu.VMEM((2, 2, rows, dim), BF),
            pltpu.VMEM((3 * width, piece), F32),
            pltpu.VMEM((width, piece), F32),
            pltpu.VMEM((1, piece), F32),
            dma((4,)),
            dma((2, nblk)),
            dma((2, 2)),
            dma((3,)),
            dma((2, 2)),
            dma((n - 1, 2)),
            dma((n - 1, 2)),
            dma((2, n - 1, 2)),
            dma((2, n - 1, 2)),
            dma((n - 1, 2)),
            dma((n - 1, 2)),
            dma((4, n - 1, 2)),
            dma((4, n - 1, 2)),
            dma((half,)),
            dma((half,)),
            dma((half - 1,)),
            dma((half - 1,)),
            dma((n - 1,)),
            dma((n - 1,)),
        ],
        compiler_params=pltpu.CompilerParams(
            collective_id=1, has_side_effects=True, vmem_limit_bytes=60 * 1024 * 1024
        ),
        name="layer",
    )(
        hist_len,
        states.reshape(total, dim),
        cotangent.reshape(total, dim),
        norm_gain,
        wqkv,
        wout,
    )
    att, gst, gq, go, gg = settle((att, gst, gq, go, gg))
    return (
        att.reshape(states.shape),
        gst.reshape(states.shape),
        gq.reshape(3, heads, size, piece).transpose(3, 0, 1, 2),
        go.reshape(heads, size, piece),
        gg.reshape(piece),
    )


def solution(mesh):
    placed = (
        P("dp", None, None),
        P("dp"),
        P(),
        P(None, None, "mp", None),
        P("mp", None, None),
        P("dp", None, None),
    )
    return jax.shard_map(
        functools.partial(body, mesh.shape["dp"], mesh.shape["mp"]),
        mesh=mesh,
        in_specs=placed,
        out_specs=(
            P("dp", None, None),
            P("dp", None, None),
            P("dp", None, "mp", None),
            P("mp", None, "dp"),
            P("dp"),
        ),
        check_vma=False,
    )
```
